32 devices in a mesh: batch: 8 (over z, core), vocab: 4 (over y, x).
Axes of the slice: x: 2, y: 2, z: 4, core: 2. Of those that a mesh axis runs over, the one named last changes fastest.
Arguments:
- window_ids: int32 [3, 16, 8], P(None, 'batch'), may hold values from 0 to 16383
- pool_ids: int32 [3, 16, 8], P(None, 'batch'), may hold values from 0 to 16383
- accepted: int32 [2, 16], P(None, 'batch'), may hold values from 1 to 8
- converged: int32 [2, 16], P(None, 'batch'), may hold values 0 or 1
- cache_lens: int32 [16], P('batch'), may hold values from 1 to 128
- table: bfloat16 [16384, 4608], P(('batch', 'vocab')), may hold values from -0.29882812 to 0.29882812
- attn_gain: float32 [4608], replicated, may hold values from 0.25 to 1.75
- post_gain: float32 [4608], replicated, may hold values from 0.25 to 1.75
- final_gain: float32 [4608], replicated, may hold values from 0.25 to 1.75
- w_query: bfloat16 [4608, 1024], P(None, 'vocab'), may hold values from -0.09375 to 0.09375
- w_key: bfloat16 [4608, 512], P(None, 'vocab'), may hold values from -0.09375 to 0.09375
- w_value: bfloat16 [4608, 512], P(None, 'vocab'), may hold values from -0.09375 to 0.09375
- w_out: bfloat16 [1024, 4608], P('vocab'), may hold values from -0.1875 to 0.1875
- cache_keys: bfloat16 [16, 4, 128, 128], P('batch', 'vocab'), may hold values from -6 to 6
- cache_values: bfloat16 [16, 4, 128, 128], P('batch', 'vocab'), may hold values from -6 to 6
Outputs:
- log_total: float32 [3, 16, 8], P(None, 'batch')
- best_logit: float32 [3, 16, 8], P(None, 'batch')
- pool_score: float32 [3, 16, 8], P(None, 'batch')
The draws below stay inside these ranges and needn't reach their ends.
Inputs may be any that keep to these rules, and one draw needn't show every extreme that they name: `converged`: 1 marks a window at its fixed point, whose tokens are all accepted.
All inputs are finite; a program needn't handle non-finite values. No bound on the sum of `converged` on one device may be relied on, other than what follows from the above.
Results may differ from the reference program's by a relative error of at most 0.00036.
Values may be sent and summed in bfloat16 or wider, within the bound.
No kernel may reach another device: no remote copies, remote signals or barrier semaphores. Data moves between devices by JAX's collectives and lax.ppermute only.
A program may use at most 128 MiB of HBM per device.

```python
import math
import jax
import jax.numpy as jnp
from jax import lax

D = 4608
HD = 128
KVH = 4
HEADS = 8
VOCAB = 16384
BATCH = 16
W = 8
CACHE = 128
ITERS = 3


def with_ends(entries, rng, least, largest):
    shape = entries.shape
    place = [jax.random.randint(jax.random.fold_in(rng, axis), (), 0, shape[axis]) for axis in range(len(shape))]
    entries = entries.at[tuple(place)].set(least)
    longest = shape.index(max(shape))
    place[longest] = (place[longest] + 1) % shape[longest]
    return entries.at[tuple(place)].set(largest)


def block_levels(key, extent, split, least, high):
    def one(axis_at, parts):
        steps = jax.random.uniform(jax.random.fold_in(jax.random.fold_in(key, 6), axis_at), (parts,), jnp.float32, least / len(split), high / len(split))
        return jnp.repeat(jnp.exp(steps), extent[axis_at] // parts).reshape((-1,) + (1,) * (len(extent) - axis_at - 1))

    factor_of = one(*split[0])
    for cut in split[1:]:
        factor_of = factor_of * one(*cut)
    return factor_of


def bell_draw(stream_key, shape, scale, limit, cuts=(), held_as=jnp.bfloat16):
    entries = jax.random.normal(stream_key, shape, jnp.float32) * scale
    if len(cuts) > 0:
        entries = block_levels(stream_key, shape, cuts, -0.22, 0.18) * entries
    return jnp.clip(entries, min=-limit, max=limit).astype(held_as)


def setup_inputs(seed: int = 0) -> dict:
    splits = jax.random.split(jax.random.key(seed), 16)
    window_ids = with_ends(jax.random.randint(splits[0], (ITERS, BATCH, W), 0, VOCAB), jax.random.fold_in(splits[0], 1), 0, VOCAB - 1).astype(jnp.int32)
    pool_ids = with_ends(jax.random.randint(splits[1], (ITERS, BATCH, W), 0, VOCAB), jax.random.fold_in(splits[1], 1), 0, VOCAB - 1).astype(jnp.int32)
    accepted = with_ends(jax.random.randint(splits[2], (ITERS - 1, BATCH), 1, W + 1), jax.random.fold_in(splits[2], 1), 1, W).astype(jnp.int32)
    converged = with_ends((jax.random.randint(splits[3], (ITERS - 1, BATCH), 0, 4) < 1).astype(jnp.int32), jax.random.fold_in(splits[3], 1), 0, 1)
    cache_lens = with_ends(jax.random.randint(splits[4], (BATCH,), 1, CACHE + 1), jax.random.fold_in(splits[4], 1), 1, CACHE).astype(jnp.int32)
    table = bell_draw(splits[5], (VOCAB, D), 0.045, 0.29882812, ((0, 32),))
    attn_gain = jnp.clip(1.0 + 0.15 * jax.random.normal(splits[6], (D,), jnp.float32), 0.25, 1.75)
    post_gain = jnp.clip(1.0 + 0.15 * jax.random.normal(splits[7], (D,), jnp.float32), 0.25, 1.75)
    final_gain = jnp.clip(1.0 + 0.15 * jax.random.normal(splits[8], (D,), jnp.float32), 0.25, 1.75)
    w_query = bell_draw(splits[9], (D, HEADS * HD), D ** -0.5, 0.09375, ((1, 4),))
    w_key = bell_draw(splits[10], (D, KVH * HD), D ** -0.5, 0.09375, ((1, 4),))
    w_value = bell_draw(splits[11], (D, KVH * HD), D ** -0.5, 0.09375, ((1, 4),))
    w_out = bell_draw(splits[12], (HEADS * HD, D), (HEADS * HD) ** -0.5, 0.1875, ((0, 4),))
    cache_keys = bell_draw(splits[13], (BATCH, KVH, CACHE, HD), 1.0, 6.0, ((0, 8), (1, 4)))
    cache_values = bell_draw(splits[14], (BATCH, KVH, CACHE, HD), 1.0, 6.0, ((0, 8), (1, 4)))
    return dict(window_ids=window_ids, pool_ids=pool_ids, accepted=accepted, converged=converged, cache_lens=cache_lens, table=table, attn_gain=attn_gain, post_gain=post_gain, final_gain=final_gain, w_query=w_query, w_key=w_key, w_value=w_value, w_out=w_out, cache_keys=cache_keys, cache_values=cache_values)


epsilon = 1e-06
query_scalar = 144.0
score_cap = 50.0
logit_cap = 30.0

def normalize(values_in, gain):
    return values_in * lax.rsqrt(lax.optimization_barrier(jnp.mean(values_in * values_in, axis=-1, keepdims=True)) + epsilon) * gain

def rotate(values_in, positions):
    half_size = values_in.shape[-1] // 2
    freqs = 10000.0 ** (-jnp.arange(half_size, dtype=jnp.float32) / half_size)
    angles = positions.astype(jnp.float32)[..., None] * freqs
    cosine = jnp.cos(angles)
    sine = jnp.sin(angles)
    first_half = values_in[..., :half_size]
    second_half = values_in[..., half_size:]
    return jnp.concatenate([first_half * cosine - second_half * sine, second_half * cosine + first_half * sine], axis=-1)

def attend(queries, key_rows, value_rows, visible):
    scores = jnp.einsum('bwhgd,bhld->bhgwl', queries.astype(jnp.float32), key_rows.astype(jnp.float32))
    scores = score_cap * jnp.tanh(scores / score_cap)
    weights = jnp.where(visible[:, None, None], jnp.exp(scores), 0.0)
    weight_sum = lax.optimization_barrier(jnp.sum(weights, axis=-1, keepdims=True))
    rounded = lax.optimization_barrier(weights.astype(jnp.bfloat16))
    summed = jnp.einsum('bhgwl,bhld->bwhgd', rounded.astype(jnp.float32), value_rows.astype(jnp.float32))
    return (summed / jnp.moveaxis(weight_sum, 3, 1)).astype(jnp.bfloat16)

def reference(window_ids, pool_ids, accepted, converged, cache_lens, table, attn_gain, post_gain, final_gain, w_query, w_key, w_value, w_out, cache_keys, cache_values):
    taken = jnp.where(converged == 1, W, accepted).astype(jnp.int32)
    offset = cache_lens.astype(jnp.int32)
    slots = jnp.arange(W, dtype=jnp.int32)
    cache_visible = jnp.arange(CACHE, dtype=jnp.int32)[None, None, :] < cache_lens[:, None, None]
    own_visible = slots[None, None, :] <= slots[None, :, None]
    key_list = [cache_keys]
    value_list = [cache_values]
    mask_list = [jnp.broadcast_to(cache_visible, (BATCH, W, CACHE))]
    totals_out = []
    best_out = []
    score_out = []
    for step in range(ITERS):
        embedded = table[window_ids[step]].astype(jnp.float32) * math.sqrt(D)
        normed = normalize(embedded, attn_gain).astype(jnp.bfloat16).reshape(BATCH * W, D)
        positions = (offset[:, None] + slots[None, :])[:, :, None]
        queries = jnp.dot(normed, w_query, preferred_element_type=jnp.float32).reshape(BATCH, W, HEADS, HD)
        queries = (rotate(queries, positions) / math.sqrt(query_scalar)).astype(jnp.bfloat16).reshape(BATCH, W, KVH, 2, HD)
        keys_now = jnp.dot(normed, w_key, preferred_element_type=jnp.float32).reshape(BATCH, W, KVH, HD)
        keys_now = rotate(keys_now, positions).astype(jnp.bfloat16).transpose(0, 2, 1, 3)
        values_now = jnp.dot(normed, w_value, preferred_element_type=jnp.float32).reshape(BATCH, W, KVH, HD)
        values_now = values_now.astype(jnp.bfloat16).transpose(0, 2, 1, 3)
        all_keys = jnp.concatenate(key_list + [keys_now], axis=2)
        all_values = jnp.concatenate(value_list + [values_now], axis=2)
        visible = jnp.concatenate(mask_list + [jnp.broadcast_to(own_visible, (BATCH, W, W))], axis=2)
        attended = attend(queries, all_keys, all_values, visible).reshape(BATCH * W, HEADS * HD)
        branch = jnp.dot(attended, w_out, preferred_element_type=jnp.float32)
        hidden = embedded.reshape(BATCH * W, D) + normalize(branch, post_gain)
        final_rows = normalize(hidden, final_gain).astype(jnp.bfloat16)
        logits = logit_cap * jnp.tanh(jnp.dot(final_rows, table.T, preferred_element_type=jnp.float32) / logit_cap)
        log_sum = jnp.log(lax.optimization_barrier(jnp.sum(jnp.exp(logits), axis=-1)))
        best = lax.optimization_barrier(jnp.max(logits, axis=-1))
        picked = jnp.take_along_axis(logits, pool_ids[step].reshape(BATCH * W, 1).astype(jnp.int32), axis=1)[:, 0]
        totals_out.append(log_sum.reshape(BATCH, W))
        best_out.append(best.reshape(BATCH, W))
        score_out.append((picked - log_sum).reshape(BATCH, W))
        if step + 1 < ITERS:
            key_list.append(keys_now)
            value_list.append(values_now)
            mask_list.append(jnp.broadcast_to(slots[None, None, :] < taken[step][:, None, None], (BATCH, W, W)))
            offset = offset + taken[step]
    return (jnp.stack(totals_out), jnp.stack(best_out), jnp.stack(score_out))
```

```python
import math

import jax
import jax.numpy as jnp
from jax import lax
from jax.experimental import pallas as pl
from jax.experimental.pallas import tpu as pltpu
from jax.sharding import PartitionSpec as P

epsilon = 1e-06
query_scalar = 144.0
score_cap = 50.0
logit_cap = 30.0
slots_sent = 8


def normalize(values_in, gain):
    return (
        values_in
        * lax.rsqrt(jnp.mean(values_in * values_in, axis=-1, keepdims=True) + epsilon)
        * gain
    )


def rotate(values_in, positions):
    half_size = values_in.shape[-1] // 2
    freqs = 10000.0 ** (-jnp.arange(half_size, dtype=jnp.float32) / half_size)
    angles = positions.astype(jnp.float32)[..., None] * freqs
    cosine = jnp.cos(angles)
    sine = jnp.sin(angles)
    first_half = values_in[..., :half_size]
    second_half = values_in[..., half_size:]
    return jnp.concatenate(
        [first_half * cosine - second_half * sine, second_half * cosine + first_half * sine],
        axis=-1,
    )


def slot_hits(ids, first, extent, first_slot):
    size = ids.shape[-1]
    inside = (ids >= first) & (ids < first + extent)
    before = lax.broadcasted_iota(jnp.int32, (size, size), 0) < lax.broadcasted_iota(
        jnp.int32, (size, size), 1
    )
    rank = jnp.dot(
        jnp.broadcast_to(jnp.where(inside, 1.0, 0.0), (slots_sent, size)),
        jnp.where(before, 1.0, 0.0),
        preferred_element_type=jnp.float32,
    )
    slots = lax.broadcasted_iota(jnp.int32, (slots_sent, size), 0) + first_slot
    return (rank == slots.astype(jnp.float32)) & inside


def send_kernel(scalars, ids, table, sent):
    first = scalars[0]
    vocab_rows = table.shape[0]
    lanes = lax.broadcasted_iota(jnp.int32, (slots_sent, vocab_rows), 1)
    one_hots = []
    for at in range(ids.shape[0]):
        at_ids = ids[at : at + 1, :]
        hits = slot_hits(at_ids, first, vocab_rows, scalars[1])
        picked = jnp.sum(
            jnp.where(hits, (at_ids - first + 1).astype(jnp.float32), 0.0), axis=1, keepdims=True
        )
        one_hots.append(
            jnp.where(picked.astype(jnp.int32) - 1 == lanes, 1.0, 0.0).astype(jnp.float32)
        )
    one_hot = jnp.concatenate(one_hots, axis=0).astype(jnp.bfloat16)
    sent[...] = jnp.dot(one_hot, table[...], preferred_element_type=jnp.float32).astype(
        jnp.bfloat16
    )


def place_kernel(scalars, ids, *refs):
    parts, placed = refs[:-1], refs[-1]
    hits = []
    for at in range(len(parts)):
        hits.append(
            jnp.where(slot_hits(ids[0:1, :], scalars[2 + at], scalars[0], scalars[1]), 1.0, 0.0)
        )
    values = jnp.concatenate([part[...].astype(jnp.float32) for part in parts], axis=0)
    placed[...] = lax.dot_general(
        jnp.concatenate(hits, axis=0).astype(jnp.bfloat16),
        values.astype(jnp.bfloat16),
        (((0,), (0,)), ((), ())),
        preferred_element_type=jnp.float32,
    ).astype(jnp.bfloat16)


def bits_of(size):
    return [1 << place for place in range(size.bit_length() - 1)]


def per_device(
    window_ids,
    pool_ids,
    accepted,
    converged,
    cache_lens,
    table,
    attn_gain,
    post_gain,
    final_gain,
    w_query,
    w_key,
    w_value,
    w_out,
    cache_keys,
    cache_values,
):
    iter_count, local_batch, width = window_ids.shape
    vocab_rows, model_width = table.shape
    head_size = cache_keys.shape[3]
    kv_local = cache_keys.shape[1]
    cache_slots = cache_keys.shape[2]
    rows = iter_count * local_batch * width
    batch_devices = lax.axis_size("batch")
    vocab_devices = lax.axis_size("vocab")
    all_devices = batch_devices * vocab_devices
    b_index = lax.axis_index("batch")
    v_index = lax.axis_index("vocab")
    core = b_index % 2
    batch_bits = bits_of(batch_devices)
    vocab_bits = bits_of(vocab_devices)
    chunk = rows // vocab_devices

    def batch_swap(value, mask):
        return lax.ppermute(value, "batch", [(at, at ^ mask) for at in range(batch_devices)])

    def mixed_swap(value, step):
        pairs = []
        for at in range(all_devices):
            b_at, v_at = divmod(at, vocab_devices)
            bit = vocab_bits[step] if b_at % 2 == 0 else vocab_bits[-1 - step]
            pairs.append((at, b_at * vocab_devices + (v_at ^ bit)))
        return lax.ppermute(value, ("batch", "vocab"), pairs)

    def owners(at_vocab, at_core):
        order = jnp.arange(vocab_devices, dtype=jnp.int32)
        total = jnp.zeros_like(order)
        last = len(vocab_bits) - 1
        for step in range(len(vocab_bits)):
            bit = jnp.where(at_core == 0, vocab_bits[step], vocab_bits[last - step])
            total = total ^ jnp.where((order >> (last - step)) & 1, bit, 0)
        return total ^ at_vocab

    own_ids = jnp.stack(
        [
            window_ids.transpose(1, 0, 2).reshape(rows),
            pool_ids.transpose(1, 0, 2).reshape(rows),
        ]
    )[None]
    all_ids = own_ids
    for bit in batch_bits:
        all_ids = jnp.concatenate([all_ids, batch_swap(all_ids, bit)], axis=0)
    token_ids = all_ids[:, 0]
    pool_all = all_ids[:, 1]
    first_id = (b_index * vocab_devices + v_index) * vocab_rows

    relative = jnp.arange(batch_devices, dtype=jnp.int32)
    source_first = ((b_index ^ relative) * vocab_devices + v_index) * vocab_rows
    vocab_iota = jnp.arange(vocab_rows, dtype=jnp.int32)
    smem = pl.BlockSpec(memory_space=pltpu.SMEM)
    vmem = pl.BlockSpec(memory_space=pltpu.VMEM)

    def exchange(first_slot):
        sent = pl.pallas_call(
            send_kernel,
            out_shape=jax.ShapeDtypeStruct((batch_devices * slots_sent, model_width), jnp.bfloat16),
            in_specs=[smem, vmem, vmem],
            out_specs=vmem,
            name="send_rows",
            cost_estimate=pl.CostEstimate(
                flops=2 * batch_devices * slots_sent * vocab_rows * model_width,
                bytes_accessed=2 * vocab_rows * model_width,
                transcendentals=0,
            ),
        )(jnp.stack([first_id, first_slot]), token_ids, table)
        got = [sent[:slots_sent]]
        for mask in range(1, batch_devices):
            got.append(batch_swap(sent[mask * slots_sent : (mask + 1) * slots_sent], mask))
        scalars = jnp.concatenate([jnp.stack([jnp.int32(vocab_rows), first_slot]), source_first])
        return pl.pallas_call(
            place_kernel,
            out_shape=jax.ShapeDtypeStruct((rows, model_width), jnp.bfloat16),
            in_specs=[smem, vmem] + [vmem] * batch_devices,
            out_specs=vmem,
            name="place_rows",
        )(scalars, token_ids[:1], *got)

    owner_ids = token_ids // vocab_rows
    counts = jnp.sum(
        jnp.where(
            owner_ids[:, :, None] == jnp.arange(all_devices, dtype=jnp.int32)[None, None, :], 1, 0
        ),
        axis=1,
    )
    most = jnp.max(counts)
    gathered = exchange(jnp.int32(0))
    _, gathered = lax.while_loop(
        lambda state: state[0] < most,
        lambda state: (state[0] + slots_sent, state[1] + exchange(state[0])),
        (jnp.int32(slots_sent), gathered),
    )
    for step in range(len(vocab_bits)):
        gathered = gathered + mixed_swap(gathered, step)

    embedded = gathered.astype(jnp.float32) * math.sqrt(model_width)
    normed = normalize(embedded, attn_gain).astype(jnp.bfloat16)
    taken = jnp.where(converged == 1, width, accepted)
    starts = [cache_lens]
    for step in range(iter_count - 1):
        starts.append(starts[-1] + taken[step])
    window_slots = jnp.arange(width, dtype=jnp.int32)
    positions = jnp.stack(starts, axis=1)[:, :, None] + window_slots
    tokens = iter_count * width
    positions = positions.reshape(local_batch, tokens, 1)
    queries = jnp.dot(normed, w_query, preferred_element_type=jnp.float32).reshape(
        local_batch, tokens, 2 * kv_local, head_size
    )
    queries = (rotate(queries, positions) / math.sqrt(query_scalar)).astype(jnp.bfloat16)
    queries = queries.reshape(local_batch, tokens, kv_local, 2, head_size)
    keys_now = jnp.dot(normed, w_key, preferred_element_type=jnp.float32).reshape(
        local_batch, tokens, kv_local, head_size
    )
    keys_now = rotate(keys_now, positions).astype(jnp.bfloat16).transpose(0, 2, 1, 3)
    values_now = jnp.dot(normed, w_value, preferred_element_type=jnp.float32).reshape(
        local_batch, tokens, kv_local, head_size
    )
    values_now = values_now.astype(jnp.bfloat16).transpose(0, 2, 1, 3)
    all_keys = jnp.concatenate([cache_keys, keys_now], axis=2)
    all_values = jnp.concatenate([cache_values, values_now], axis=2)
    token_window = jnp.arange(tokens) // width
    token_slot = jnp.arange(tokens) % width
    taken_full = jnp.concatenate([taken, jnp.zeros_like(taken[:1])], axis=0)
    kept = token_slot[None, :] < jnp.repeat(taken_full.T, width, axis=1)
    earlier = token_window[None, :] < token_window[:, None]
    same = (token_window[None, :] == token_window[:, None]) & (
        token_slot[None, :] <= token_slot[:, None]
    )
    visible_now = (earlier[None] & kept[:, None, :]) | same[None]
    cache_visible = jnp.arange(cache_slots)[None, None, :] < cache_lens[:, None, None]
    visible = jnp.concatenate(
        [jnp.broadcast_to(cache_visible, (local_batch, tokens, cache_slots)), visible_now], axis=2
    )
    scores = jnp.einsum("bwhgd,bhld->bhgwl", queries, all_keys, preferred_element_type=jnp.float32)
    scores = score_cap * jnp.tanh(scores / score_cap)
    weights = jnp.where(visible[:, None, None], jnp.exp(scores), 0.0)
    weight_sum = jnp.sum(weights, axis=-1, keepdims=True)
    summed = jnp.einsum(
        "bhgwl,bhld->bwhgd",
        weights.astype(jnp.bfloat16),
        all_values,
        preferred_element_type=jnp.float32,
    )
    attended = (summed / jnp.moveaxis(weight_sum, 3, 1)).astype(jnp.bfloat16)
    attended = attended.reshape(rows, 2 * kv_local * head_size)

    chunk_owner = owners(v_index, core)
    row_order = (chunk_owner[:, None] * chunk + jnp.arange(chunk, dtype=jnp.int32)).reshape(rows)
    reorder = row_order[:, None] == jnp.arange(rows, dtype=jnp.int32)[None, :]
    reorder_b = reorder.astype(jnp.bfloat16)
    attended = jnp.dot(reorder_b, attended, preferred_element_type=jnp.float32).astype(jnp.bfloat16)
    own_embedded = jnp.dot(reorder_b[:chunk], gathered, preferred_element_type=jnp.float32)
    own_embedded = own_embedded * math.sqrt(model_width)
    branch = jnp.dot(attended, w_out, preferred_element_type=jnp.float32)
    for step in range(len(vocab_bits)):
        half = branch.shape[0] // 2
        branch = branch[:half] + mixed_swap(branch[half:].astype(jnp.bfloat16), step).astype(
            jnp.float32
        )
    hidden = own_embedded + normalize(branch, post_gain)
    final_rows = normalize(hidden, final_gain).astype(jnp.bfloat16)

    far_bits = batch_devices // 2
    blocks = [final_rows]
    for mask in range(1, far_bits):
        blocks.append(batch_swap(final_rows, 2 * mask))
    own_blocks = [jnp.concatenate(blocks, axis=0)]
    for step in range(len(vocab_bits)):
        step = len(vocab_bits) - 1 - step
        own_blocks = own_blocks + [mixed_swap(block, step) for block in own_blocks]
    other_blocks = [batch_swap(block, 1) for block in own_blocks]

    def pools_for(at_core):
        order = owners(v_index, core ^ at_core)
        at_rows = order[:, None] * chunk + jnp.arange(chunk, dtype=jnp.int32)
        pools = pool_all[at_core::2]
        hit = at_rows[None, :, :, None] == jnp.arange(rows, dtype=jnp.int32)
        ids = jnp.sum(jnp.where(hit, pools[:, None, None, :], 0), axis=-1)
        return ids.transpose(1, 0, 2).reshape(vocab_devices, -1) - first_id

    def scored(final_part, pools):
        raw = lax.dot_general(
            final_part, table, (((1,), (1,)), ((), ())), preferred_element_type=jnp.float32
        )
        logits = logit_cap * jnp.tanh(raw / logit_cap)
        sums = jnp.sum(jnp.exp(logits), axis=-1)
        chosen = jnp.sum(jnp.where(vocab_iota[None, :] == pools[:, None], logits, 0.0), axis=-1)
        return jnp.stack([sums, chosen, jnp.max(logits, axis=-1)])

    def joined(first, second):
        return jnp.concatenate([first[:2] + second[:2], jnp.maximum(first[2:], second[2:])])

    def scored_blocks(parts, pools):
        return jnp.stack([scored(part, pools[at]) for at, part in enumerate(parts)], axis=1)

    own_scores = scored_blocks(own_blocks, pools_for(0))
    other_scores = scored_blocks(other_blocks, pools_for(1))
    total = joined(own_scores, batch_swap(other_scores, 1))
    total = total.reshape(3, vocab_devices, far_bits, chunk)
    for bit in reversed(bits_of(far_bits)):
        half = total.shape[2] // 2
        total = joined(total[:, :, :half], batch_swap(total[:, :, half:], 2 * bit))
    total = total.reshape(3, vocab_devices, chunk)
    for step in range(len(vocab_bits)):
        lead = 1 << step
        split = total.reshape(3, lead, 2, vocab_devices // lead // 2, chunk)
        flipped = split[:, :, ::-1].reshape(total.shape)
        total = joined(total, mixed_swap(flipped, step))
    total = total.reshape(3, rows)
    total = jnp.sum(jnp.where(reorder[None], total[:, :, None], 0.0), axis=1)
    log_sum = jnp.log(total[0])

    def placed(values):
        return values.reshape(local_batch, iter_count, width).transpose(1, 0, 2)

    return (placed(log_sum), placed(total[2]), placed(total[1] - log_sum))


def solution(mesh):
    return jax.shard_map(
        per_device,
        mesh=mesh,
        in_specs=(
            P(None, "batch", None),
            P(None, "batch", None),
            P(None, "batch"),
            P(None, "batch"),
            P("batch"),
            P(("batch", "vocab"), None),
            P(),
            P(),
            P(),
            P(None, "vocab"),
            P(None, "vocab"),
            P(None, "vocab"),
            P("vocab", None),
            P("batch", "vocab", None, None),
            P("batch", "vocab", None, None),
        ),
        out_specs=(P(None, "batch", None), P(None, "batch", None), P(None, "batch", None)),
        check_vma=False,
    )
```

```python
import functools
import math

import jax
import jax.numpy as jnp
import numpy as np
from jax import lax
from jax.experimental import pallas as pl
from jax.experimental.pallas import tpu as pltpu
from jax.sharding import PartitionSpec as P


epsilon = 1e-06
query_scalar = 144.0
score_cap = 50.0
logit_cap = 30.0
slots_sent = 12
half_count = 2
lane_count = 128


f32 = jnp.float32
bf16 = jnp.bfloat16
smem = pl.BlockSpec(memory_space=pltpu.SMEM)
vmem = pl.BlockSpec(memory_space=pltpu.VMEM)


def normalize(values_in, gain):
    return (
        values_in
        * lax.rsqrt(jnp.mean(values_in * values_in, axis=-1, keepdims=True) + epsilon)
        * gain
    )


def bits_of(size):
    return [1 << place for place in range(size.bit_length() - 1)]


def iota(shape, dimension):
    return lax.broadcasted_iota(jnp.int32, shape, dimension)


def owner_of(order, at_vocab, at_core):
    vocab_bits = bits_of(lax.axis_size("vocab"))
    last = len(vocab_bits) - 1
    total = order ^ order
    for step in range(len(vocab_bits)):
        bit = jnp.where(at_core == 0, vocab_bits[step], vocab_bits[last - step])
        total = total ^ (((order >> (last - step)) & 1) * bit)
    return total ^ at_vocab


def side_by_side(ref, first, count, found, stride):
    parts = [ref[pl.ds(first + at, found, stride=stride), :] for at in range(count)]
    return jnp.concatenate(parts, axis=1)


def slot_hits(ids, first, extent, first_slot):
    size = ids.shape[-1]
    inside = (ids >= first) & (ids < first + extent)
    before = iota((size, size), 0) < iota((size, size), 1)
    rank = jnp.dot(
        jnp.broadcast_to(jnp.where(inside, 1.0, 0.0), (8, size)),
        jnp.where(before, 1.0, 0.0),
        preferred_element_type=f32,
    )[:1]
    slots = iota((half_count * slots_sent, size), 0) % slots_sent + first_slot
    return (rank == slots.astype(f32)) & inside


def of_chip(ids, at, at_core):
    mine, other = ids[at : at + 1, :], ids[at + 1 : at + 2, :]
    first = jnp.where(at_core == 0, mine, other)
    second = jnp.where(at_core == 0, other, mine)
    return jnp.concatenate([first, second], axis=1)


def pack_kernel(windows, pools, ids, held, done):
    copies = [
        pltpu.make_async_copy(ref, held.at[at], done.at[at])
        for at, ref in enumerate((windows, pools))
    ]
    for copy in copies:
        copy.start()
    for copy in copies:
        copy.wait()
    groups = windows.shape[0] * windows.shape[1]
    for kind in range(2):
        for at in range(windows.shape[0]):
            first = kind * groups + at * windows.shape[1]
            ids[first : first + windows.shape[1], :] = held[kind, at]


def send_kernel(first_slot, ids, table, *outs):
    batch_devices = lax.axis_size("batch")
    vocab_devices = lax.axis_size("vocab")
    far = batch_devices // 2
    at_core = lax.axis_index("batch") % 2
    vocab_rows, model_width = table.shape
    first = (lax.axis_index("batch") * vocab_devices + lax.axis_index("vocab")) * vocab_rows
    sent, pools, most = outs[:far], outs[far], outs[far + 1]
    stride = ids.shape[0] // batch_devices
    tokens = side_by_side(ids, 0, stride // 2, batch_devices, stride)
    pools[...] = side_by_side(ids, stride // 2, stride // 2, batch_devices, stride)
    block = half_count * slots_sent
    lanes = iota((block, vocab_rows), 1)
    one_hots = []
    for at in range(far):
        at_ids = of_chip(tokens, 2 * at, at_core)
        hits = slot_hits(at_ids, first, vocab_rows, first_slot[0])
        picked = jnp.sum(
            jnp.where(hits, (at_ids - first + 1).astype(f32), 0.0), axis=1, keepdims=True
        )
        one_hots.append(jnp.where(picked.astype(jnp.int32) - 1 == lanes, 1.0, 0.0).astype(f32))
    one_hot = jnp.concatenate(one_hots, axis=0)
    half_of = (iota(one_hot.shape, 0) % block) // slots_sent
    wide = model_width // half_count
    rows = jnp.zeros((one_hot.shape[0], wide), f32)
    for half in range(half_count):
        rows = rows + jnp.dot(
            jnp.where(half_of == half, one_hot, 0.0).astype(bf16),
            table[:, half * wide : (half + 1) * wide],
            preferred_element_type=f32,
        )
    for at in range(far):
        sent[at][...] = rows[at * block : (at + 1) * block].astype(bf16)
    owner = lax.div(tokens, jnp.full_like(tokens, vocab_rows)).astype(f32)
    columns = jnp.transpose(owner)
    largest = jnp.zeros((1, owner.shape[1]), f32)
    for at in range(batch_devices):
        equal = jnp.zeros((owner.shape[1], owner.shape[1]), f32)
        for other in (at, at ^ 1):
            equal = equal + jnp.where(
                columns[:, other : other + 1] == owner[at : at + 1, :], 1.0, 0.0
            )
        largest = jnp.maximum(largest, jnp.sum(equal, axis=0, keepdims=True))
    most[0] = jnp.max(largest).astype(jnp.int32)


def place_kernel(first_slot, vocab_rows, ids, *refs):
    parts, placed = refs[:-half_count], refs[-half_count:]
    batch_devices = lax.axis_size("batch")
    at_core = lax.axis_index("batch") % 2
    stride = ids.shape[0] // batch_devices
    tokens = side_by_side(ids, 0, stride // 2, 2, stride)
    size = tokens.shape[1]
    chip = of_chip(tokens, 0, at_core)
    hits = []
    for at in range(len(parts)):
        other = at // (batch_devices // 2)
        relative = 2 * (at % (batch_devices // 2)) + other
        source = (lax.axis_index("batch") ^ relative) * lax.axis_size("vocab")
        first = (source + lax.axis_index("vocab")) * vocab_rows
        found = jnp.where(slot_hits(chip, first, vocab_rows, first_slot[0]), 1.0, 0.0)
        hits.append(jnp.where(at_core == 0, found[:, :size], found[:, size:]))
    hits = jnp.concatenate(hits, axis=0)
    half_of = (iota(hits.shape, 0) % (half_count * slots_sent)) // slots_sent
    values = jnp.concatenate([part[...].astype(f32) for part in parts], axis=0).astype(bf16)
    for half in range(half_count):
        placed[half][...] = lax.dot_general(
            jnp.where(half_of == half, hits, 0.0).astype(bf16),
            values,
            (((0,), (0,)), ((), ())),
            preferred_element_type=f32,
        ).astype(bf16)


def turn_kernel(accepted, converged, cache_lens, freqs, signs, cosine, sine):
    windows = accepted.shape[0] + 1
    width = cosine.shape[0] // (windows * cache_lens.shape[0])
    positions = []
    for at in range(windows):
        for at_batch in range(cache_lens.shape[0]):
            start = cache_lens[at_batch]
            for before in range(at):
                start = start + jnp.where(
                    converged[before, at_batch] == 1, width, accepted[before, at_batch]
                )
            positions.append(iota((width, cosine.shape[1]), 0) + start)
    angles = jnp.concatenate(positions, axis=0).astype(f32) * freqs[...]
    cosine[...] = jnp.cos(angles)
    sine[...] = jnp.sin(angles) * signs[...]


def attend_kernel(
    accepted,
    converged,
    cache_lens,
    kept_first,
    kept_second,
    got_first,
    got_second,
    cosine,
    sine,
    attn_gain,
    w_query,
    w_key,
    w_value,
    w_out,
    cache_keys,
    cache_values,
    keep,
    send,
    own,
):
    rows = got_first.shape[0]
    model_width = w_query.shape[0]
    local_batch, kv_local, cache_slots, head_size = cache_keys.shape
    iter_count = accepted.shape[0] + 1
    width = rows // (iter_count * local_batch)
    tokens = iter_count * width
    chunk = own.shape[0]
    at_vocab = lax.axis_index("vocab")
    at_core = lax.axis_index("batch") % 2
    gathered = jnp.concatenate(
        [
            kept_first[...].astype(f32) + got_first[...].astype(f32),
            kept_second[...].astype(f32) + got_second[...].astype(f32),
        ],
        axis=1,
    )
    embedded = gathered * math.sqrt(model_width)
    normed = normalize(embedded, attn_gain[...]).astype(bf16)

    def turned(values):
        return values * cosine[...] + pltpu.roll(values, head_size // 2, 1) * sine[...]

    queries = jnp.dot(normed, w_query[...], preferred_element_type=f32)
    keys = jnp.dot(normed, w_key[...], preferred_element_type=f32)
    values = jnp.dot(normed, w_value[...], preferred_element_type=f32)

    def of_sequence(array, at_batch, head):
        starts = [(at * local_batch + at_batch) * width for at in range(iter_count)]
        lanes = slice(head * head_size, (head + 1) * head_size)
        return jnp.concatenate([array[at : at + width, lanes] for at in starts], axis=0)

    nt = (((1,), (1,)), ((), ()))
    attended_rows = []
    turned_queries = [
        turned(queries[:, head * head_size : (head + 1) * head_size]) / math.sqrt(query_scalar)
        for head in range(2 * kv_local)
    ]
    turned_keys = [
        turned(keys[:, head * head_size : (head + 1) * head_size]) for head in range(kv_local)
    ]
    for at_batch in range(local_batch):
        taken = [
            jnp.where(converged[at, at_batch] == 1, width, accepted[at, at_batch])
            for at in range(iter_count - 1)
        ]
        query_at = iota((2 * tokens, tokens), 0) % tokens
        key_at = iota((2 * tokens, tokens), 1)
        key_taken = jnp.zeros((2 * tokens, tokens), jnp.int32)
        for at in range(iter_count - 1):
            key_taken = jnp.where(key_at // width == at, taken[at], key_taken)
        earlier = (key_at // width < query_at // width) & (key_at % width < key_taken)
        same = (key_at // width == query_at // width) & (key_at <= query_at)
        visible_now = earlier | same
        visible_cache = iota((2 * tokens, cache_slots), 1) < cache_lens[at_batch]
        heads = []
        for head in range(kv_local):
            pair = jnp.concatenate(
                [
                    of_sequence(turned_queries[2 * head], at_batch, 0),
                    of_sequence(turned_queries[2 * head + 1], at_batch, 0),
                ],
                axis=0,
            ).astype(bf16)
            keys_now = of_sequence(turned_keys[head], at_batch, 0).astype(bf16)
            values_now = of_sequence(values, at_batch, head).astype(bf16)

            def weigh(scores, visible):
                scores = score_cap * jnp.tanh(scores / score_cap)
                return jnp.where(visible, jnp.exp(scores), 0.0)

            from_cache = weigh(
                lax.dot_general(pair, cache_keys[at_batch, head], nt, preferred_element_type=f32),
                visible_cache,
            )
            from_now = weigh(
                lax.dot_general(pair, keys_now, nt, preferred_element_type=f32), visible_now
            )
            weight_sum = jnp.sum(from_cache, axis=1, keepdims=True) + jnp.sum(
                from_now, axis=1, keepdims=True
            )
            summed = jnp.dot(
                from_cache.astype(bf16), cache_values[at_batch, head], preferred_element_type=f32
            ) + jnp.dot(from_now.astype(bf16), values_now, preferred_element_type=f32)
            attended = summed / weight_sum
            heads += [attended[:tokens], attended[tokens:]]
        attended_rows.append(jnp.concatenate(heads, axis=1))
    attended = jnp.concatenate(attended_rows, axis=0).astype(bf16)

    ordered = iota((rows, rows), 0)
    wanted = owner_of(ordered // chunk, at_vocab, at_core) * chunk + ordered % chunk
    place = iota((rows, rows), 1)
    at_batch = place // tokens
    at_window = (place % tokens) // width
    standing = (at_window * local_batch + at_batch) * width + place % width
    by_sequence = jnp.where(wanted == standing, 1.0, 0.0).astype(bf16)
    by_window = jnp.where(wanted == place, 1.0, 0.0)[:chunk].astype(bf16)
    own[...] = jnp.dot(by_window, gathered.astype(bf16), preferred_element_type=f32).astype(bf16)
    attended = jnp.dot(by_sequence, attended, preferred_element_type=f32).astype(bf16)
    half = rows // 2
    send[...] = jnp.dot(attended[half:], w_out[...], preferred_element_type=f32).astype(bf16)
    keep[...] = jnp.dot(attended[:half], w_out[...], preferred_element_type=f32)


def halve_kernel(kept, got, keep, send):
    half = keep.shape[0]
    total = kept[...] + got[...].astype(f32)
    keep[...] = total[:half]
    send[...] = total[half:].astype(bf16)


def final_kernel(kept, got, own, post_gain, final_gain, final):
    model_width = kept.shape[1]
    branch = kept[...] + got[...].astype(f32)
    embedded = own[...].astype(f32) * math.sqrt(model_width)
    hidden = embedded + normalize(branch, post_gain[...])
    rows = normalize(hidden, final_gain[...])
    wide = model_width // half_count
    final[...] = jnp.concatenate(
        [rows[:, half * wide : (half + 1) * wide] for half in range(half_count)], axis=0
    ).astype(bf16)


def assemble_kernel(*refs):
    parts, block = refs[:-1], refs[-1]
    wide = parts[0].shape[1]
    chunk = parts[0].shape[0] // half_count
    values = [part[...].astype(f32) for part in parts]
    for half in range(half_count):
        block[:, half * wide : (half + 1) * wide] = jnp.concatenate(
            [value[half * chunk : (half + 1) * chunk] for value in values], axis=0
        ).astype(bf16)


def score_blocks(blocks, core_of, order_of, tables, pools):
    vocab_rows = sum(table.shape[0] for table in tables)
    vocab_devices = lax.axis_size("vocab")
    at_vocab = lax.axis_index("vocab")
    at_core = lax.axis_index("batch") % 2
    far = lax.axis_size("batch") // 2
    block_rows = blocks[0][0].shape[0]
    chunk = block_rows // far
    first = (lax.axis_index("batch") * vocab_devices + at_vocab) * vocab_rows
    wanted = []
    for other, order in zip(core_of, order_of):
        owner = owner_of(jnp.int32(order), at_vocab, at_core ^ other)
        parts = []
        for at in range(far):
            pool = pools[2 * at + other : 2 * at + other + 1, :]
            part = jnp.zeros((1, chunk), jnp.int32)
            for place in range(vocab_devices):
                part = jnp.where(
                    owner == place, pool[:, place * chunk : (place + 1) * chunk], part
                )
            parts.append(part)
        wanted.append(jnp.concatenate(parts, axis=1))
    wanted = jnp.concatenate(wanted, axis=1) - first
    values = [
        jnp.concatenate([block[half][...] for block in blocks], axis=0)
        for half in range(len(blocks[0]))
    ]
    wide = values[0].shape[1]
    sums, chosen, largest = [], [], []
    for table in tables:
        raw = jnp.zeros((table.shape[0], values[0].shape[0]), f32)
        for half, value in enumerate(values):
            raw = raw + lax.dot_general(
                table[:, half * wide : (half + 1) * wide],
                value,
                (((1,), (1,)), ((), ())),
                preferred_element_type=f32,
            )
        logits = logit_cap * jnp.tanh(raw / logit_cap)
        sums.append(jnp.sum(jnp.exp(logits), axis=0, keepdims=True))
        hit = iota(logits.shape, 0) == wanted
        chosen.append(jnp.sum(jnp.where(hit, logits, 0.0), axis=0, keepdims=True))
        largest.append(jnp.max(logits, axis=0, keepdims=True))
        wanted = wanted - table.shape[0]
    sums, chosen = sum(sums), sum(chosen)
    top = largest[0]
    for row in largest[1:]:
        top = jnp.maximum(top, row)
    largest = top
    return [
        [row[:, at * block_rows : (at + 1) * block_rows] for at in range(len(blocks))]
        for row in (sums, chosen, largest)
    ]


def score_kernel(orders, halves, parts, *refs):
    pools, scores = refs[-2:]
    tables = refs[len(refs) - 2 - parts : -2]
    blocks = [refs[at * halves : (at + 1) * halves] for at in range(2 * len(orders))]
    found = score_blocks(blocks, [0] * len(orders) + [1] * len(orders), orders * 2, tables, pools)
    for kind in range(3):
        for at in range(len(blocks)):
            row = kind * len(blocks) + at
            scores[row : row + 1, :] = found[kind][at]


def late_kernel(orders, halves, parts, *refs):
    vocab_devices = lax.axis_size("vocab")
    at_vocab = lax.axis_index("vocab")
    at_batch = lax.axis_index("batch")
    far = lax.axis_size("batch") // 2
    message = refs[-1]
    scores = refs[-1 - len(orders) : -1]
    pools = refs[-2 - len(orders)]
    tables = refs[2 * halves : 2 * halves + parts]
    blocks = [refs[:halves], refs[halves : 2 * halves]]
    block_rows = blocks[0][0].shape[0]
    chunk = block_rows // far
    late = score_blocks(blocks, [0, 1], [vocab_devices - 1] * 2, tables, pools)
    for other in range(2):
        kinds = []
        for kind in range(3):
            found = []
            for group, score in zip(orders, scores):
                row = (kind * 2 + other) * len(group)
                found += [score[row + at : row + at + 1, :] for at in range(len(group))]
            found.append(late[kind][other])
            owners = [
                owner_of(jnp.int32(at), at_vocab, (at_batch % 2) ^ other)
                for at in range(vocab_devices)
            ]
            chunks = []
            for place in range(vocab_devices):
                total = jnp.zeros_like(found[0])
                for at in range(vocab_devices):
                    total = jnp.where(owners[at] == place, found[at], total)
                chunks.append(total)
            kinds.append(jnp.concatenate(chunks, axis=0))
        for at in range(far):
            pieces = [kind[:, at * chunk : (at + 1) * chunk] for kind in kinds]
            pieces.append(jnp.zeros((vocab_devices, lane_count - 3 * chunk), f32))
            piece = jnp.concatenate(pieces, axis=1)
            piece = jnp.concatenate([piece] * vocab_devices, axis=0)
            target = at_batch ^ (2 * at + other)
            size = vocab_devices * vocab_devices
            message[pl.ds(pl.multiple_of(target * size, 8), size), :] = piece


def result_kernel(got, log_total, best_logit, pool_score):
    vocab_devices = lax.axis_size("vocab")
    iter_count, local_batch, width = log_total.shape
    rows = iter_count * local_batch * width
    chunk = rows // vocab_devices
    step = max(8, vocab_devices)
    added = got[0:step, :]
    largest = added
    for at in range(1, got.shape[0] // step):
        part = got[at * step : (at + 1) * step, :]
        added = added + part
        largest = jnp.maximum(largest, part)
    total, top = added[:vocab_devices], largest[:vocab_devices]
    for at in range(1, step // vocab_devices):
        total = total + added[at * vocab_devices : (at + 1) * vocab_devices]
        top = jnp.maximum(top, largest[at * vocab_devices : (at + 1) * vocab_devices])

    def flat(array, kind):
        return jnp.concatenate(
            [array[at : at + 1, kind * chunk : (kind + 1) * chunk] for at in range(vocab_devices)],
            axis=1,
        )

    log_sum = jnp.log(flat(total, 0))
    for ref, found in (
        (log_total, log_sum),
        (best_logit, flat(top, 2)),
        (pool_score, flat(total, 1) - log_sum),
    ):
        for at in range(iter_count):
            for at_batch in range(local_batch):
                start = (at * local_batch + at_batch) * width
                ref[at, at_batch : at_batch + 1, :] = found[:, start : start + width]


def call(kernel, shapes, in_specs, out_specs, flops=0, scratch=(), grant=8):
    return pl.pallas_call(
        kernel,
        out_shape=shapes,
        in_specs=in_specs,
        out_specs=out_specs,
        scratch_shapes=scratch,
        compiler_params=pltpu.CompilerParams(vmem_limit_bytes=grant << 20),
        cost_estimate=pl.CostEstimate(flops=flops, bytes_accessed=flops // 100, transcendentals=0),
    )


def per_device(
    window_ids,
    pool_ids,
    accepted,
    converged,
    cache_lens,
    table,
    attn_gain,
    post_gain,
    final_gain,
    w_query,
    w_key,
    w_value,
    w_out,
    cache_keys,
    cache_values,
):
    iter_count, local_batch, width = window_ids.shape
    vocab_rows, model_width = table.shape
    head_size = cache_keys.shape[3]
    groups = iter_count * local_batch
    rows = groups * width
    batch_devices = lax.axis_size("batch")
    vocab_devices = lax.axis_size("vocab")
    all_devices = batch_devices * vocab_devices
    vocab_bits = bits_of(vocab_devices)
    chunk = rows // vocab_devices
    far = batch_devices // 2

    def shape(*dims, kind=bf16):
        return jax.ShapeDtypeStruct(dims, kind)

    def batch_swap(value, mask):
        return lax.ppermute(value, "batch", [(at, at ^ mask) for at in range(batch_devices)])

    def mixed_swap(value, step):
        pairs = []
        for at in range(all_devices):
            b_at, v_at = divmod(at, vocab_devices)
            bit = vocab_bits[step] if b_at % 2 == 0 else vocab_bits[-1 - step]
            pairs.append((at, b_at * vocab_devices + (v_at ^ bit)))
        return lax.ppermute(value, ("batch", "vocab"), pairs)

    in_hbm = pl.BlockSpec(memory_space=pltpu.HBM)
    own_ids = call(
        pack_kernel,
        shape(2 * groups, width, kind=jnp.int32),
        [in_hbm] * 2,
        vmem,
        scratch=[
            pltpu.VMEM((2, iter_count, local_batch, width), jnp.int32),
            pltpu.SemaphoreType.DMA((2,)),
        ],
        grant=2,
    )(window_ids, pool_ids)
    all_ids = own_ids
    for bit in bits_of(batch_devices):
        all_ids = jnp.concatenate([all_ids, batch_swap(all_ids, bit)], axis=0)

    def exchange(first_slot):
        *sent, pools, most = call(
            send_kernel,
            [shape(half_count * slots_sent, model_width // half_count)] * far
            + [shape(batch_devices, rows, kind=jnp.int32), shape(1, kind=jnp.int32)],
            [smem, vmem, vmem],
            [vmem] * (far + 1) + [smem],
            flops=2 * batch_devices * slots_sent * vocab_rows * model_width,
            grant=10,
        )(first_slot, all_ids, table)
        got = [sent[0]]
        for mask in range(1, far):
            got.append(batch_swap(sent[mask], 2 * mask))
        other = [batch_swap(part, 1) for part in got]
        placed = call(
            lambda slot, *refs: place_kernel(slot, vocab_rows, *refs),
            [shape(rows, model_width // half_count)] * half_count,
            [smem, vmem] + [vmem] * batch_devices,
            [vmem] * half_count,
            flops=10**8,
        )(first_slot, all_ids, *got, *other)
        return placed, pools, most

    start_slot = jnp.zeros((1,), jnp.int32)
    gathered, pools, most = exchange(start_slot)

    def another_round(state):
        later = state[0] + slots_sent
        return later, [old + new for old, new in zip(state[1], exchange(later)[0])]

    _, gathered = lax.while_loop(
        lambda state: state[0][0] + slots_sent < most[0], another_round, (start_slot, list(gathered))
    )
    for step in range(len(vocab_bits) - 1):
        received = []
        for half in range(half_count):
            received.append(mixed_swap(gathered[half], step))
        gathered = [kept + got for kept, got in zip(gathered, received)]
    received = []
    for half in range(half_count):
        received.append(mixed_swap(gathered[half], len(vocab_bits) - 1))

    half_size = head_size // 2
    freqs = np.float32(10000.0) ** (-np.arange(half_size, dtype=np.float32) / half_size)
    signs = np.concatenate([-np.ones(half_size), np.ones(half_size)]).astype(np.float32)
    cosine, sine = call(
        turn_kernel,
        [shape(rows, head_size, kind=f32)] * 2,
        [smem] * 3 + [vmem] * 2,
        [vmem] * 2,
        flops=10**7,
    )(
        accepted,
        converged,
        cache_lens,
        jnp.asarray(np.concatenate([freqs, freqs])[None]),
        jnp.asarray(signs[None]),
    )

    wide = w_query.shape[1] + w_key.shape[1] + w_value.shape[1]
    keep, send, own = call(
        attend_kernel,
        [
            shape(rows // 2, model_width, kind=f32),
            shape(rows // 2, model_width),
            shape(chunk, model_width),
        ],
        [smem] * 3 + [vmem] * 13,
        [vmem] * 3,
        flops=2 * rows * model_width * (wide + w_out.shape[0]),
        grant=20,
    )(
        accepted,
        converged,
        cache_lens,
        *gathered,
        *received,
        cosine,
        sine,
        attn_gain[None],
        w_query,
        w_key,
        w_value,
        w_out,
        cache_keys,
        cache_values,
    )
    for step in range(len(vocab_bits) - 1):
        half = keep.shape[0] // 2
        keep, send = call(
            halve_kernel,
            [shape(half, model_width, kind=f32), shape(half, model_width)],
            [vmem] * 2,
            [vmem] * 2,
        )(keep, mixed_swap(send, step))
    final = call(
        final_kernel,
        shape(half_count * chunk, model_width // half_count),
        [vmem] * 5,
        vmem,
    )(keep, mixed_swap(send, len(vocab_bits) - 1), own, post_gain[None], final_gain[None])

    parts = [final]
    for mask in range(1, far):
        parts.append(batch_swap(final, 2 * mask))
    blocks = [
        call(assemble_kernel, shape(far * chunk, model_width), [vmem] * far, vmem)(*parts)
    ]
    for step in range(len(vocab_bits)):
        step = len(vocab_bits) - 1 - step
        for at in range(len(blocks)):
            blocks.append(mixed_swap(blocks[at], step))
    halves = 1
    own_blocks = [blocks]
    other_blocks = [[batch_swap(each, 1) for each in blocks]]

    per_block = 2 * far * chunk * vocab_rows * model_width

    def halves_of(blocks, orders):
        return [blocks[half][order] for order in orders for half in range(halves)]

    groups_of = [[0], list(range(1, vocab_devices - 1))]
    scores = []
    for orders in groups_of:
        inputs = halves_of(own_blocks, orders) + halves_of(other_blocks, orders)
        scores.append(
            call(
                functools.partial(score_kernel, orders, halves, 1),
                shape(6 * len(orders), far * chunk, kind=f32),
                [vmem] * (len(inputs) + 1 + 1),
                vmem,
                flops=2 * per_block * len(orders),
            )(*inputs, table, pools)
        )
    last = [vocab_devices - 1]
    message = call(
        functools.partial(late_kernel, groups_of, halves, 1),
        shape(all_devices * vocab_devices, lane_count, kind=f32),
        [vmem] * (2 * halves + 1 + 1 + len(scores)),
        vmem,
        flops=2 * per_block,
    )(*halves_of(own_blocks, last), *halves_of(other_blocks, last), table, pools, *scores)
    totals = lax.all_to_all(message, ("batch", "vocab"), 0, 0, tiled=True)
    return tuple(
        call(
            result_kernel,
            [shape(iter_count, local_batch, width, kind=f32)] * 3,
            [vmem],
            [vmem] * 3,
        )(totals)
    )


def solution(mesh):
    return jax.shard_map(
        per_device,
        mesh=mesh,
        in_specs=(
            P(None, "batch", None),
            P(None, "batch", None),
            P(None, "batch"),
            P(None, "batch"),
            P("batch"),
            P(("batch", "vocab"), None),
            P(),
            P(),
            P(),
            P(None, "vocab"),
            P(None, "vocab"),
            P(None, "vocab"),
            P("vocab", None),
            P("batch", "vocab", None, None),
            P("batch", "vocab", None, None),
        ),
        out_specs=(P(None, "batch", None), P(None, "batch", None), P(None, "batch", None)),
        check_vma=False,
    )
```

```python
import functools
import math

import jax
import jax.numpy as jnp
import numpy as np
from jax import lax
from jax.experimental import pallas as pl
from jax.experimental.pallas import tpu as pltpu
from jax.sharding import PartitionSpec as P


epsilon = 1e-06
query_scalar = 144.0
score_cap = 50.0
logit_cap = 30.0
slots_sent = 12
half_count = 2
lane_count = 128


f32 = jnp.float32
bf16 = jnp.bfloat16
smem = pl.BlockSpec(memory_space=pltpu.SMEM)
vmem = pl.BlockSpec(memory_space=pltpu.VMEM)


def normalize(values_in, gain):
    return (
        values_in
        * lax.rsqrt(jnp.mean(values_in * values_in, axis=-1, keepdims=True) + epsilon)
        * gain
    )


def bits_of(size):
    return [1 << place for place in range(size.bit_length() - 1)]


def iota(shape, dimension):
    return lax.broadcasted_iota(jnp.int32, shape, dimension)


def owner_of(order, at_vocab, at_core):
    vocab_bits = bits_of(lax.axis_size("vocab"))
    last = len(vocab_bits) - 1
    total = order ^ order
    for step in range(len(vocab_bits)):
        bit = jnp.where(at_core == 0, vocab_bits[step], vocab_bits[last - step])
        total = total ^ (((order >> (last - step)) & 1) * bit)
    return total ^ at_vocab


def side_by_side(ref, first, count, found, stride):
    parts = [ref[pl.ds(first + at, found, stride=stride), :] for at in range(count)]
    return jnp.concatenate(parts, axis=1)


def slot_hits(ids, first, extent, first_slot):
    size = ids.shape[-1]
    inside = (ids >= first) & (ids < first + extent)
    before = iota((size, size), 0) < iota((size, size), 1)
    rank = jnp.dot(
        jnp.broadcast_to(jnp.where(inside, 1.0, 0.0), (8, size)),
        jnp.where(before, 1.0, 0.0),
        preferred_element_type=f32,
    )[:1]
    slots = iota((half_count * slots_sent, size), 0) % slots_sent + first_slot
    return (rank == slots.astype(f32)) & inside


def of_chip(ids, at, at_core):
    mine, other = ids[at : at + 1, :], ids[at + 1 : at + 2, :]
    first = jnp.where(at_core == 0, mine, other)
    second = jnp.where(at_core == 0, other, mine)
    return jnp.concatenate([first, second], axis=1)


def pack_kernel(windows, pools, ids, held, done):
    copies = [
        pltpu.make_async_copy(ref, held.at[at], done.at[at])
        for at, ref in enumerate((windows, pools))
    ]
    for copy in copies:
        copy.start()
    for copy in copies:
        copy.wait()
    groups = windows.shape[0] * windows.shape[1]
    for kind in range(2):
        for at in range(windows.shape[0]):
            first = kind * groups + at * windows.shape[1]
            ids[first : first + windows.shape[1], :] = held[kind, at]


def load_kernel(start, source, target, done):
    copy = pltpu.make_async_copy(source.at[pl.ds(start, target.shape[0])], target, done)
    copy.start()
    copy.wait()


def send_kernel(first_slot, ids, upper, lower, *outs):
    batch_devices = lax.axis_size("batch")
    vocab_devices = lax.axis_size("vocab")
    far = batch_devices // 2
    at_core = lax.axis_index("batch") % 2
    part_rows, model_width = upper.shape
    vocab_rows = 2 * part_rows
    first = (lax.axis_index("batch") * vocab_devices + lax.axis_index("vocab")) * vocab_rows
    sent, pools, most = outs[:far], outs[far], outs[far + 1]
    stride = ids.shape[0] // batch_devices
    tokens = side_by_side(ids, 0, stride // 2, batch_devices, stride)
    pools[...] = side_by_side(ids, stride // 2, stride // 2, batch_devices, stride)
    block = half_count * slots_sent
    lanes = iota((block, vocab_rows), 1)
    one_hots = []
    for at in range(far):
        at_ids = of_chip(tokens, 2 * at, at_core)
        hits = slot_hits(at_ids, first, vocab_rows, first_slot[0])
        picked = jnp.sum(
            jnp.where(hits, (at_ids - first + 1).astype(f32), 0.0), axis=1, keepdims=True
        )
        one_hots.append(jnp.where(picked.astype(jnp.int32) - 1 == lanes, 1.0, 0.0).astype(f32))
    one_hot = jnp.concatenate(one_hots, axis=0)
    half_of = (iota(one_hot.shape, 0) % block) // slots_sent
    wide = model_width // half_count
    rows = jnp.zeros((one_hot.shape[0], wide), f32)
    for half in range(half_count):
        chosen = jnp.where(half_of == half, one_hot, 0.0).astype(bf16)
        for at, part in enumerate((upper, lower)):
            rows = rows + jnp.dot(
                chosen[:, at * part_rows : (at + 1) * part_rows],
                part[:, half * wide : (half + 1) * wide],
                preferred_element_type=f32,
            )
    for at in range(far):
        sent[at][...] = rows[at * block : (at + 1) * block].astype(bf16)
    owner = lax.div(tokens, jnp.full_like(tokens, vocab_rows)).astype(f32)
    columns = jnp.transpose(owner)
    largest = jnp.zeros((1, owner.shape[1]), f32)
    for at in range(batch_devices):
        equal = jnp.zeros((owner.shape[1], owner.shape[1]), f32)
        for other in (at, at ^ 1):
            equal = equal + jnp.where(
                columns[:, other : other + 1] == owner[at : at + 1, :], 1.0, 0.0
            )
        largest = jnp.maximum(largest, jnp.sum(equal, axis=0, keepdims=True))
    most[0] = jnp.max(largest).astype(jnp.int32)


def place_kernel(first_slot, vocab_rows, ids, *refs):
    parts, placed = refs[:-half_count], refs[-half_count:]
    batch_devices = lax.axis_size("batch")
    at_core = lax.axis_index("batch") % 2
    stride = ids.shape[0] // batch_devices
    tokens = side_by_side(ids, 0, stride // 2, 2, stride)
    size = tokens.shape[1]
    chip = of_chip(tokens, 0, at_core)
    hits = []
    for at in range(len(parts)):
        other = at // (batch_devices // 2)
        relative = 2 * (at % (batch_devices // 2)) + other
        source = (lax.axis_index("batch") ^ relative) * lax.axis_size("vocab")
        first = (source + lax.axis_index("vocab")) * vocab_rows
        found = jnp.where(slot_hits(chip, first, vocab_rows, first_slot[0]), 1.0, 0.0)
        hits.append(jnp.where(at_core == 0, found[:, :size], found[:, size:]))
    hits = jnp.concatenate(hits, axis=0)
    half_of = (iota(hits.shape, 0) % (half_count * slots_sent)) // slots_sent
    values = jnp.concatenate([part[...].astype(f32) for part in parts], axis=0).astype(bf16)
    for half in range(half_count):
        placed[half][...] = lax.dot_general(
            jnp.where(half_of == half, hits, 0.0).astype(bf16),
            values,
            (((0,), (0,)), ((), ())),
            preferred_element_type=f32,
        ).astype(bf16)


def turn_kernel(accepted, converged, cache_lens, freqs, signs, cosine, sine):
    windows = accepted.shape[0] + 1
    width = cosine.shape[0] // (windows * cache_lens.shape[0])
    positions = []
    for at in range(windows):
        for at_batch in range(cache_lens.shape[0]):
            start = cache_lens[at_batch]
            for before in range(at):
                start = start + jnp.where(
                    converged[before, at_batch] == 1, width, accepted[before, at_batch]
                )
            positions.append(iota((width, cosine.shape[1]), 0) + start)
    angles = jnp.concatenate(positions, axis=0).astype(f32) * freqs[...]
    cosine[...] = jnp.cos(angles)
    sine[...] = jnp.sin(angles) * signs[...]


def stacked(values):
    wide = values.shape[1] // half_count
    return jnp.concatenate(
        [values[:, half * wide : (half + 1) * wide] for half in range(half_count)], axis=0
    )


def attend_kernel(
    accepted,
    converged,
    cache_lens,
    kept_first,
    kept_second,
    got_first,
    got_second,
    cosine,
    sine,
    attn_gain,
    w_query,
    w_key,
    w_value,
    w_out,
    cache_keys,
    cache_values,
    keep,
    own,
    *sends,
):
    rows = got_first.shape[0]
    model_width = w_query.shape[0]
    local_batch, kv_local, cache_slots, head_size = cache_keys.shape
    iter_count = accepted.shape[0] + 1
    width = rows // (iter_count * local_batch)
    tokens = iter_count * width
    chunk = own.shape[0]
    at_vocab = lax.axis_index("vocab")
    gathered = jnp.concatenate(
        [
            kept_first[...].astype(f32) + got_first[...].astype(f32),
            kept_second[...].astype(f32) + got_second[...].astype(f32),
        ],
        axis=1,
    )
    embedded = gathered * math.sqrt(model_width)
    normed = normalize(embedded, attn_gain[...]).astype(bf16)

    def turned(values):
        return values * cosine[...] + pltpu.roll(values, head_size // 2, 1) * sine[...]

    queries = jnp.dot(normed, w_query[...], preferred_element_type=f32)
    keys = jnp.dot(normed, w_key[...], preferred_element_type=f32)
    values = jnp.dot(normed, w_value[...], preferred_element_type=f32)

    def of_sequence(array, at_batch, head):
        starts = [(at * local_batch + at_batch) * width for at in range(iter_count)]
        lanes = slice(head * head_size, (head + 1) * head_size)
        return jnp.concatenate([array[at : at + width, lanes] for at in starts], axis=0)

    nt = (((1,), (1,)), ((), ()))
    attended_rows = []
    turned_queries = [
        turned(queries[:, head * head_size : (head + 1) * head_size]) / math.sqrt(query_scalar)
        for head in range(2 * kv_local)
    ]
    turned_keys = [
        turned(keys[:, head * head_size : (head + 1) * head_size]) for head in range(kv_local)
    ]
    for at_batch in range(local_batch):
        taken = [
            jnp.where(converged[at, at_batch] == 1, width, accepted[at, at_batch])
            for at in range(iter_count - 1)
        ]
        query_at = iota((2 * tokens, tokens), 0) % tokens
        key_at = iota((2 * tokens, tokens), 1)
        key_taken = jnp.zeros((2 * tokens, tokens), jnp.int32)
        for at in range(iter_count - 1):
            key_taken = jnp.where(key_at // width == at, taken[at], key_taken)
        earlier = (key_at // width < query_at // width) & (key_at % width < key_taken)
        same = (key_at // width == query_at // width) & (key_at <= query_at)
        visible_now = earlier | same
        visible_cache = iota((2 * tokens, cache_slots), 1) < cache_lens[at_batch]
        heads = []
        for head in range(kv_local):
            pair = jnp.concatenate(
                [
                    of_sequence(turned_queries[2 * head], at_batch, 0),
                    of_sequence(turned_queries[2 * head + 1], at_batch, 0),
                ],
                axis=0,
            ).astype(bf16)
            keys_now = of_sequence(turned_keys[head], at_batch, 0).astype(bf16)
            values_now = of_sequence(values, at_batch, head).astype(bf16)

            def weigh(scores, visible):
                scores = score_cap * jnp.tanh(scores / score_cap)
                return jnp.where(visible, jnp.exp(scores), 0.0)

            from_cache = weigh(
                lax.dot_general(pair, cache_keys[at_batch, head], nt, preferred_element_type=f32),
                visible_cache,
            )
            from_now = weigh(
                lax.dot_general(pair, keys_now, nt, preferred_element_type=f32), visible_now
            )
            weight_sum = jnp.sum(from_cache, axis=1, keepdims=True) + jnp.sum(
                from_now, axis=1, keepdims=True
            )
            summed = jnp.dot(
                from_cache.astype(bf16), cache_values[at_batch, head], preferred_element_type=f32
            ) + jnp.dot(from_now.astype(bf16), values_now, preferred_element_type=f32)
            attended = summed / weight_sum
            heads += [attended[:tokens], attended[tokens:]]
        attended_rows.append(jnp.concatenate(heads, axis=1))
    attended = jnp.concatenate(attended_rows, axis=0).astype(bf16)

    ordered = iota((rows, rows), 0)
    wanted = ((ordered // chunk) ^ at_vocab) * chunk + ordered % chunk
    place = iota((rows, rows), 1)
    at_batch = place // tokens
    at_window = (place % tokens) // width
    standing = (at_window * local_batch + at_batch) * width + place % width
    by_sequence = jnp.where(wanted == standing, 1.0, 0.0).astype(bf16)
    by_window = jnp.where(wanted == place, 1.0, 0.0)[:chunk].astype(bf16)
    own[...] = jnp.dot(by_window, gathered.astype(bf16), preferred_element_type=f32).astype(bf16)
    attended = jnp.dot(by_sequence, attended, preferred_element_type=f32).astype(bf16)
    branch = jnp.dot(attended, w_out[...], preferred_element_type=f32)
    keep[...] = branch[:chunk]
    for at, ref in enumerate(sends):
        ref[...] = stacked(branch[(at + 1) * chunk : (at + 2) * chunk]).astype(bf16)


def final_kernel(kept, own, post_gain, final_gain, *refs):
    parts, final = refs[:-1], refs[-1]
    chunk, model_width = kept.shape
    total = jnp.zeros((half_count * chunk, model_width // half_count), f32)
    for part in parts:
        total = total + part[...].astype(f32)
    branch = kept[...] + jnp.concatenate(
        [total[half * chunk : (half + 1) * chunk] for half in range(half_count)], axis=1
    )
    embedded = own[...].astype(f32) * math.sqrt(model_width)
    hidden = embedded + normalize(branch, post_gain[...])
    final[...] = stacked(normalize(hidden, final_gain[...])).astype(bf16)


def join_kernel(*refs):
    parts, joint = refs[:-1], refs[-1]
    joint[...] = jnp.concatenate([part[...].astype(f32) for part in parts], axis=0).astype(bf16)


def half_of_block(near, distant, half):
    size = near.shape[0]
    chunk = size // half_count
    count = distant.shape[0] // size
    parts = [near[...].astype(f32)[half * chunk : (half + 1) * chunk]]
    values = distant[...].astype(f32)
    for at in range(count):
        start = at * size + half * chunk
        parts.append(values[start : start + chunk])
    return jnp.concatenate(parts, axis=0)


def score_blocks(blocks, core_of, order_of, tables, pools):
    vocab_rows = sum(table.shape[0] for table in tables)
    vocab_devices = lax.axis_size("vocab")
    at_vocab = lax.axis_index("vocab")
    at_core = lax.axis_index("batch") % 2
    far = lax.axis_size("batch") // 2
    chunk = blocks[0][0].shape[0] // half_count
    block_rows = chunk * far
    first = (lax.axis_index("batch") * vocab_devices + at_vocab) * vocab_rows
    wanted = []
    for other, order in zip(core_of, order_of):
        owner = owner_of(jnp.int32(order), at_vocab, at_core ^ other)
        parts = []
        for at in range(far):
            pool = pools[2 * at + other : 2 * at + other + 1, :]
            part = jnp.zeros((1, chunk), jnp.int32)
            for place in range(vocab_devices):
                part = jnp.where(
                    owner == place, pool[:, place * chunk : (place + 1) * chunk], part
                )
            parts.append(part)
        wanted.append(jnp.concatenate(parts, axis=1))
    wanted = jnp.concatenate(wanted, axis=1) - first
    values = [
        jnp.concatenate([half_of_block(*block, half) for block in blocks], axis=0).astype(bf16)
        for half in range(half_count)
    ]
    wide = values[0].shape[1]
    sums, chosen, largest = [], [], []
    for table in tables:
        raw = jnp.zeros((table.shape[0], values[0].shape[0]), f32)
        for half, value in enumerate(values):
            raw = raw + lax.dot_general(
                table[:, half * wide : (half + 1) * wide],
                value,
                (((1,), (1,)), ((), ())),
                preferred_element_type=f32,
            )
        logits = logit_cap * jnp.tanh(raw / logit_cap)
        sums.append(jnp.sum(jnp.exp(logits), axis=0, keepdims=True))
        hit = iota(logits.shape, 0) == wanted
        chosen.append(jnp.sum(jnp.where(hit, logits, 0.0), axis=0, keepdims=True))
        largest.append(jnp.max(logits, axis=0, keepdims=True))
        wanted = wanted - table.shape[0]
    sums, chosen = sum(sums), sum(chosen)
    top = largest[0]
    for row in largest[1:]:
        top = jnp.maximum(top, row)
    largest = top
    return [
        [row[:, at * block_rows : (at + 1) * block_rows] for at in range(len(blocks))]
        for row in (sums, chosen, largest)
    ]


def score_kernel(orders, halves, parts, *refs):
    pools, scores = refs[-2:]
    tables = refs[len(refs) - 2 - parts : -2]
    count = (len(refs) - parts - 2) // halves
    blocks = [refs[at * halves : (at + 1) * halves] for at in range(count)]
    cores = [0, 1] if len(blocks) > len(orders) else [0]
    core_of = [core for core in cores for _ in orders]
    found = score_blocks(blocks, core_of, orders * len(cores), tables, pools)
    for kind in range(3):
        for at in range(len(blocks)):
            row = kind * len(blocks) + at
            scores[row : row + 1, :] = found[kind][at]


def late_kernel(orders, *refs):
    vocab_devices = lax.axis_size("vocab")
    at_vocab = lax.axis_index("vocab")
    at_batch = lax.axis_index("batch")
    far = lax.axis_size("batch") // 2
    message = refs[-1]
    scores = refs[-2 - len(orders) : -1]
    block, tables, pools = refs[:2], refs[2:4], refs[4]
    chunk = block[0].shape[0] // half_count
    late = score_blocks([block], [1], [vocab_devices - 1], tables, pools)
    for other in range(2):
        kinds = []
        for kind in range(3):
            found = []
            for group, score in zip(orders, scores):
                row = (kind * 2 + other) * len(group)
                found += [score[row + at : row + at + 1, :] for at in range(len(group))]
            found.append(scores[-1][kind : kind + 1, :] if other == 0 else late[kind][0])
            owners = [
                owner_of(jnp.int32(at), at_vocab, (at_batch % 2) ^ other)
                for at in range(vocab_devices)
            ]
            chunks = []
            for place in range(vocab_devices):
                total = jnp.zeros_like(found[0])
                for at in range(vocab_devices):
                    total = jnp.where(owners[at] == place, found[at], total)
                chunks.append(total)
            kinds.append(jnp.concatenate(chunks, axis=0))
        for at in range(far):
            pieces = [kind[:, at * chunk : (at + 1) * chunk] for kind in kinds]
            pieces.append(jnp.zeros((vocab_devices, lane_count - 3 * chunk), f32))
            piece = jnp.concatenate(pieces, axis=1)
            piece = jnp.concatenate([piece] * vocab_devices, axis=0)
            target = at_batch ^ (2 * at + other)
            size = vocab_devices * vocab_devices
            message[pl.ds(pl.multiple_of(target * size, 8), size), :] = piece


def result_kernel(got, log_total, best_logit, pool_score):
    vocab_devices = lax.axis_size("vocab")
    iter_count, local_batch, width = log_total.shape
    rows = iter_count * local_batch * width
    chunk = rows // vocab_devices
    step = max(8, vocab_devices)
    added = got[0:step, :]
    largest = added
    for at in range(1, got.shape[0] // step):
        part = got[at * step : (at + 1) * step, :]
        added = added + part
        largest = jnp.maximum(largest, part)
    total, top = added[:vocab_devices], largest[:vocab_devices]
    for at in range(1, step // vocab_devices):
        total = total + added[at * vocab_devices : (at + 1) * vocab_devices]
        top = jnp.maximum(top, largest[at * vocab_devices : (at + 1) * vocab_devices])

    def flat(array, kind):
        return jnp.concatenate(
            [array[at : at + 1, kind * chunk : (kind + 1) * chunk] for at in range(vocab_devices)],
            axis=1,
        )

    log_sum = jnp.log(flat(total, 0))
    for ref, found in (
        (log_total, log_sum),
        (best_logit, flat(top, 2)),
        (pool_score, flat(total, 1) - log_sum),
    ):
        for at in range(iter_count):
            for at_batch in range(local_batch):
                start = (at * local_batch + at_batch) * width
                ref[at, at_batch : at_batch + 1, :] = found[:, start : start + width]


def call(kernel, shapes, in_specs, out_specs, flops=0, scratch=(), grant=8):
    return pl.pallas_call(
        kernel,
        out_shape=shapes,
        in_specs=in_specs,
        out_specs=out_specs,
        scratch_shapes=scratch,
        compiler_params=pltpu.CompilerParams(vmem_limit_bytes=grant << 20),
        cost_estimate=pl.CostEstimate(flops=flops, bytes_accessed=flops // 100, transcendentals=0),
    )


def per_device(
    window_ids,
    pool_ids,
    accepted,
    converged,
    cache_lens,
    table,
    attn_gain,
    post_gain,
    final_gain,
    w_query,
    w_key,
    w_value,
    w_out,
    cache_keys,
    cache_values,
):
    iter_count, local_batch, width = window_ids.shape
    vocab_rows, model_width = table.shape
    head_size = cache_keys.shape[3]
    groups = iter_count * local_batch
    rows = groups * width
    batch_devices = lax.axis_size("batch")
    vocab_devices = lax.axis_size("vocab")
    all_devices = batch_devices * vocab_devices
    vocab_bits = bits_of(vocab_devices)
    chunk = rows // vocab_devices
    far = batch_devices // 2

    def shape(*dims, kind=bf16):
        return jax.ShapeDtypeStruct(dims, kind)

    def batch_swap(value, mask):
        return lax.ppermute(value, "batch", [(at, at ^ mask) for at in range(batch_devices)])

    def mixed_swap(value, step):
        pairs = []
        for at in range(all_devices):
            b_at, v_at = divmod(at, vocab_devices)
            bit = vocab_bits[step] if b_at % 2 == 0 else vocab_bits[-1 - step]
            pairs.append((at, b_at * vocab_devices + (v_at ^ bit)))
        return lax.ppermute(value, ("batch", "vocab"), pairs)

    in_hbm = pl.BlockSpec(memory_space=pltpu.HBM)
    own_ids = call(
        pack_kernel,
        shape(2 * groups, width, kind=jnp.int32),
        [in_hbm] * 2,
        vmem,
        scratch=[
            pltpu.VMEM((2, iter_count, local_batch, width), jnp.int32),
            pltpu.SemaphoreType.DMA((2,)),
        ],
        grant=60,
    )(window_ids, pool_ids)
    all_ids = own_ids
    for bit in bits_of(batch_devices):
        all_ids = jnp.concatenate([all_ids, batch_swap(all_ids, bit)], axis=0)

    part_rows = vocab_rows // 2
    tables = []
    for at in range(2):
        tables.append(
            call(
                functools.partial(load_kernel, at * part_rows),
                shape(part_rows, model_width),
                [pl.BlockSpec(memory_space=pl.ANY)],
                vmem,
                flops=10**8,
                scratch=[pltpu.SemaphoreType.DMA(())],
                grant=57,
            )(table)
        )

    def exchange(first_slot):
        *sent, pools, most = call(
            send_kernel,
            [shape(half_count * slots_sent, model_width // half_count)] * far
            + [shape(batch_devices, rows, kind=jnp.int32), shape(1, kind=jnp.int32)],
            [smem, vmem, vmem, vmem],
            [vmem] * (far + 1) + [smem],
            flops=2 * batch_devices * slots_sent * vocab_rows * model_width,
            grant=10,
        )(first_slot, all_ids, *tables)
        got = [sent[0]]
        for mask in range(1, far):
            got.append(batch_swap(sent[mask], 2 * mask))
        other = [batch_swap(part, 1) for part in got]
        placed = call(
            lambda slot, *refs: place_kernel(slot, vocab_rows, *refs),
            [shape(rows, model_width // half_count)] * half_count,
            [smem, vmem] + [vmem] * batch_devices,
            [vmem] * half_count,
            flops=10**8,
        )(first_slot, all_ids, *got, *other)
        return placed, pools, most

    start_slot = jnp.zeros((1,), jnp.int32)
    gathered, pools, most = exchange(start_slot)

    def another_round(state):
        later = state[0] + slots_sent
        return later, [old + new for old, new in zip(state[1], exchange(later)[0])]

    _, gathered = lax.while_loop(
        lambda state: state[0][0] + slots_sent < most[0], another_round, (start_slot, list(gathered))
    )
    for step in range(len(vocab_bits) - 1):
        received = []
        for half in range(half_count):
            received.append(mixed_swap(gathered[half], step))
        gathered = [kept + got for kept, got in zip(gathered, received)]
    received = []
    for half in range(half_count):
        received.append(mixed_swap(gathered[half], len(vocab_bits) - 1))

    half_size = head_size // 2
    freqs = np.float32(10000.0) ** (-np.arange(half_size, dtype=np.float32) / half_size)
    signs = np.concatenate([-np.ones(half_size), np.ones(half_size)]).astype(np.float32)
    cosine, sine = call(
        turn_kernel,
        [shape(rows, head_size, kind=f32)] * 2,
        [smem] * 3 + [vmem] * 2,
        [vmem] * 2,
        flops=10**7,
    )(
        accepted,
        converged,
        cache_lens,
        jnp.asarray(np.concatenate([freqs, freqs])[None]),
        jnp.asarray(signs[None]),
    )

    wide = w_query.shape[1] + w_key.shape[1] + w_value.shape[1]
    keep, own, *sends = call(
        attend_kernel,
        [
            shape(chunk, model_width, kind=f32),
            shape(chunk, model_width),
        ]
        + [shape(half_count * chunk, model_width // half_count)] * (vocab_devices - 1),
        [smem] * 3 + [vmem] * 13,
        [vmem] * (vocab_devices + 1),
        flops=2 * rows * model_width * (wide + w_out.shape[0]),
        grant=20,
    )(
        accepted,
        converged,
        cache_lens,
        *gathered,
        *received,
        cosine,
        sine,
        attn_gain[None],
        w_query,
        w_key,
        w_value,
        w_out,
        cache_keys,
        cache_values,
    )
    branches = []
    for at, send in enumerate(sends):
        pairs = [(place, place ^ (at + 1)) for place in range(vocab_devices)]
        branches.append(lax.ppermute(send, "vocab", pairs))
    final = call(
        final_kernel,
        shape(half_count * chunk, model_width // half_count),
        [vmem] * (len(branches) + 4),
        vmem,
    )(keep, own, post_gain[None], final_gain[None], *branches)

    parts = []
    for mask in range(1, far):
        parts.append(batch_swap(final, 2 * mask))
    joint = call(
        join_kernel,
        shape((far - 1) * half_count * chunk, model_width // half_count),
        [vmem] * (far - 1),
        vmem,
    )(*parts)
    halves = 2
    own_blocks, other_blocks = [], []
    for block in (final, joint):
        blocks = [block]
        for step in range(len(vocab_bits)):
            step = len(vocab_bits) - 1 - step
            for at in range(len(blocks)):
                blocks.append(mixed_swap(blocks[at], step))
        own_blocks.append(blocks)
        others = []
        for each in blocks:
            others.append(batch_swap(each, 1))
        other_blocks.append(others)

    per_block = 2 * far * chunk * vocab_rows * model_width

    def halves_of(blocks, orders):
        return [blocks[half][order] for order in orders for half in range(halves)]

    groups_of = [[0], list(range(1, vocab_devices - 1))]
    scores = []
    for orders in groups_of:
        inputs = halves_of(own_blocks, orders) + halves_of(other_blocks, orders)
        scores.append(
            call(
                functools.partial(score_kernel, orders, halves, 2),
                shape(6 * len(orders), far * chunk, kind=f32),
                [vmem] * (len(inputs) + 3),
                vmem,
                flops=2 * per_block * len(orders),
                grant=6 + (16 * len(orders) * far * chunk * model_width >> 20),
            )(*inputs, *tables, pools)
        )
    last = vocab_devices - 1
    scores.append(
        call(
            functools.partial(score_kernel, [last], halves, 2),
            shape(3, far * chunk, kind=f32),
            [vmem] * (halves + 3),
            vmem,
            flops=per_block,
        )(*halves_of(own_blocks, [last]), *tables, pools)
    )
    message = call(
        functools.partial(late_kernel, groups_of),
        shape(all_devices * vocab_devices, lane_count, kind=f32),
        [vmem] * (halves + 3 + len(scores)),
        vmem,
        flops=per_block,
    )(*halves_of(other_blocks, [last]), *tables, pools, *scores)
    totals = lax.all_to_all(message, ("batch", "vocab"), 0, 0, tiled=True)
    return tuple(
        call(
            result_kernel,
            [shape(iter_count, local_batch, width, kind=f32)] * 3,
            [vmem],
            [vmem] * 3,
        )(totals)
    )


def solution(mesh):
    return jax.shard_map(
        per_device,
        mesh=mesh,
        in_specs=(
            P(None, "batch", None),
            P(None, "batch", None),
            P(None, "batch"),
            P(None, "batch"),
            P("batch"),
            P(("batch", "vocab"), None),
            P(),
            P(),
            P(),
            P(None, "vocab"),
            P(None, "vocab"),
            P(None, "vocab"),
            P("vocab", None),
            P("batch", "vocab", None, None),
            P("batch", "vocab", None, None),
        ),
        out_specs=(P(None, "batch", None), P(None, "batch", None), P(None, "batch", None)),
        check_vma=False,
    )
```

```python
import functools
import math

import jax
import jax.numpy as jnp
import numpy as np
from jax import lax
from jax.experimental import pallas as pl
from jax.experimental.pallas import tpu as pltpu
from jax.sharding import PartitionSpec as P


epsilon = 1e-06
query_scalar = 144.0
score_cap = 50.0
logit_cap = 30.0
slots_sent = 12
half_count = 2
lane_count = 128


f32 = jnp.float32
bf16 = jnp.bfloat16
smem = pl.BlockSpec(memory_space=pltpu.SMEM)
vmem = pl.BlockSpec(memory_space=pltpu.VMEM)


def normalize(values_in, gain):
    return (
        values_in
        * lax.rsqrt(jnp.mean(values_in * values_in, axis=-1, keepdims=True) + epsilon)
        * gain
    )


def bits_of(size):
    return [1 << place for place in range(size.bit_length() - 1)]


def iota(shape, dimension):
    return lax.broadcasted_iota(jnp.int32, shape, dimension)


def owner_of(order, at_vocab, at_core):
    vocab_bits = bits_of(lax.axis_size("vocab"))
    last = len(vocab_bits) - 1
    total = order ^ order
    for step in range(len(vocab_bits)):
        bit = jnp.where(at_core == 0, vocab_bits[step], vocab_bits[last - step])
        total = total ^ (((order >> (last - step)) & 1) * bit)
    return total ^ at_vocab


def side_by_side(ref, first, count, found, stride):
    parts = [ref[pl.ds(first + at, found, stride=stride), :] for at in range(count)]
    return jnp.concatenate(parts, axis=1)


def slot_hits(ids, first, extent, first_slot):
    size = ids.shape[-1]
    inside = (ids >= first) & (ids < first + extent)
    before = iota((size, size), 0) < iota((size, size), 1)
    rank = jnp.dot(
        jnp.broadcast_to(jnp.where(inside, 1.0, 0.0), (8, size)),
        jnp.where(before, 1.0, 0.0),
        preferred_element_type=f32,
    )[:1]
    slots = iota((half_count * slots_sent, size), 0) % slots_sent + first_slot
    return (rank == slots.astype(f32)) & inside


def of_chip(ids, at, at_core):
    mine, other = ids[at : at + 1, :], ids[at + 1 : at + 2, :]
    first = jnp.where(at_core == 0, mine, other)
    second = jnp.where(at_core == 0, other, mine)
    return jnp.concatenate([first, second], axis=1)


def pack_kernel(windows, pools, ids, held, done):
    copies = [
        pltpu.make_async_copy(ref, held.at[at], done.at[at])
        for at, ref in enumerate((windows, pools))
    ]
    for copy in copies:
        copy.start()
    for copy in copies:
        copy.wait()
    groups = windows.shape[0] * windows.shape[1]
    for kind in range(2):
        for at in range(windows.shape[0]):
            first = kind * groups + at * windows.shape[1]
            ids[first : first + windows.shape[1], :] = held[kind, at]


def load_kernel(start, source, target, done):
    copy = pltpu.make_async_copy(source.at[pl.ds(start, target.shape[0])], target, done)
    copy.start()
    copy.wait()


def send_kernel(first_slot, ids, upper, lower, *outs):
    batch_devices = lax.axis_size("batch")
    vocab_devices = lax.axis_size("vocab")
    far = batch_devices // 2
    at_core = lax.axis_index("batch") % 2
    part_rows, model_width = upper.shape
    vocab_rows = 2 * part_rows
    first = (lax.axis_index("batch") * vocab_devices + lax.axis_index("vocab")) * vocab_rows
    sent, pools, most = outs[:far], outs[far], outs[far + 1]
    stride = ids.shape[0] // batch_devices
    tokens = side_by_side(ids, 0, stride // 2, batch_devices, stride)
    pools[...] = side_by_side(ids, stride // 2, stride // 2, batch_devices, stride)
    block = half_count * slots_sent
    lanes = iota((block, vocab_rows), 1)
    one_hots = []
    for at in range(far):
        at_ids = of_chip(tokens, 2 * at, at_core)
        hits = slot_hits(at_ids, first, vocab_rows, first_slot[0])
        picked = jnp.sum(
            jnp.where(hits, (at_ids - first + 1).astype(f32), 0.0), axis=1, keepdims=True
        )
        one_hots.append(jnp.where(picked.astype(jnp.int32) - 1 == lanes, 1.0, 0.0).astype(f32))
    one_hot = jnp.concatenate(one_hots, axis=0)
    half_of = (iota(one_hot.shape, 0) % block) // slots_sent
    wide = model_width // half_count
    rows = jnp.zeros((one_hot.shape[0], wide), f32)
    for half in range(half_count):
        chosen = jnp.where(half_of == half, one_hot, 0.0).astype(bf16)
        for at, part in enumerate((upper, lower)):
            rows = rows + jnp.dot(
                chosen[:, at * part_rows : (at + 1) * part_rows],
                part[:, half * wide : (half + 1) * wide],
                preferred_element_type=f32,
            )
    for at in range(far):
        sent[at][...] = rows[at * block : (at + 1) * block].astype(bf16)
    owner = lax.div(tokens, jnp.full_like(tokens, vocab_rows)).astype(f32)
    columns = jnp.transpose(owner)
    largest = jnp.zeros((1, owner.shape[1]), f32)
    for at in range(batch_devices):
        equal = jnp.zeros((owner.shape[1], owner.shape[1]), f32)
        for other in (at, at ^ 1):
            equal = equal + jnp.where(
                columns[:, other : other + 1] == owner[at : at + 1, :], 1.0, 0.0
            )
        largest = jnp.maximum(largest, jnp.sum(equal, axis=0, keepdims=True))
    most[0] = jnp.max(largest).astype(jnp.int32)


def place_kernel(first_slot, vocab_rows, ids, *refs):
    parts, placed = refs[:-half_count], refs[-half_count:]
    batch_devices = lax.axis_size("batch")
    at_core = lax.axis_index("batch") % 2
    stride = ids.shape[0] // batch_devices
    tokens = side_by_side(ids, 0, stride // 2, 2, stride)
    size = tokens.shape[1]
    chip = of_chip(tokens, 0, at_core)
    hits = []
    for at in range(len(parts)):
        other = at // (batch_devices // 2)
        relative = 2 * (at % (batch_devices // 2)) + other
        source = (lax.axis_index("batch") ^ relative) * lax.axis_size("vocab")
        first = (source + lax.axis_index("vocab")) * vocab_rows
        found = jnp.where(slot_hits(chip, first, vocab_rows, first_slot[0]), 1.0, 0.0)
        hits.append(jnp.where(at_core == 0, found[:, :size], found[:, size:]))
    hits = jnp.concatenate(hits, axis=0)
    half_of = (iota(hits.shape, 0) % (half_count * slots_sent)) // slots_sent
    values = jnp.concatenate([part[...].astype(f32) for part in parts], axis=0).astype(bf16)
    for half in range(half_count):
        placed[half][...] = lax.dot_general(
            jnp.where(half_of == half, hits, 0.0).astype(bf16),
            values,
            (((0,), (0,)), ((), ())),
            preferred_element_type=f32,
        ).astype(bf16)


def turn_kernel(accepted, converged, cache_lens, freqs, signs, cosine, sine):
    windows = accepted.shape[0] + 1
    width = cosine.shape[0] // (windows * cache_lens.shape[0])
    positions = []
    for at in range(windows):
        for at_batch in range(cache_lens.shape[0]):
            start = cache_lens[at_batch]
            for before in range(at):
                start = start + jnp.where(
                    converged[before, at_batch] == 1, width, accepted[before, at_batch]
                )
            positions.append(iota((width, cosine.shape[1]), 0) + start)
    angles = jnp.concatenate(positions, axis=0).astype(f32) * freqs[...]
    cosine[...] = jnp.cos(angles)
    sine[...] = jnp.sin(angles) * signs[...]


def stacked(values):
    wide = values.shape[1] // half_count
    return jnp.concatenate(
        [values[:, half * wide : (half + 1) * wide] for half in range(half_count)], axis=0
    )


def attend_kernel(
    accepted,
    converged,
    cache_lens,
    kept_first,
    kept_second,
    got_first,
    got_second,
    cosine,
    sine,
    attn_gain,
    w_query,
    w_key,
    w_value,
    w_out,
    cache_keys,
    cache_values,
    keep,
    own,
    *sends,
):
    rows = got_first.shape[0]
    model_width = w_query.shape[0]
    local_batch, kv_local, cache_slots, head_size = cache_keys.shape
    iter_count = accepted.shape[0] + 1
    width = rows // (iter_count * local_batch)
    tokens = iter_count * width
    chunk = own.shape[0]
    at_vocab = lax.axis_index("vocab")
    gathered = jnp.concatenate(
        [
            kept_first[...].astype(f32) + got_first[...].astype(f32),
            kept_second[...].astype(f32) + got_second[...].astype(f32),
        ],
        axis=1,
    )
    embedded = gathered * math.sqrt(model_width)
    normed = normalize(embedded, attn_gain[...]).astype(bf16)

    def turned(values):
        return values * cosine[...] + pltpu.roll(values, head_size // 2, 1) * sine[...]

    queries = jnp.dot(normed, w_query[...], preferred_element_type=f32)
    keys = jnp.dot(normed, w_key[...], preferred_element_type=f32)
    values = jnp.dot(normed, w_value[...], preferred_element_type=f32)

    def of_sequence(array, at_batch, head):
        starts = [(at * local_batch + at_batch) * width for at in range(iter_count)]
        lanes = slice(head * head_size, (head + 1) * head_size)
        return jnp.concatenate([array[at : at + width, lanes] for at in starts], axis=0)

    nt = (((1,), (1,)), ((), ()))
    attended_rows = []
    turned_queries = [
        turned(queries[:, head * head_size : (head + 1) * head_size]) / math.sqrt(query_scalar)
        for head in range(2 * kv_local)
    ]
    turned_keys = [
        turned(keys[:, head * head_size : (head + 1) * head_size]) for head in range(kv_local)
    ]
    for at_batch in range(local_batch):
        taken = [
            jnp.where(converged[at, at_batch] == 1, width, accepted[at, at_batch])
            for at in range(iter_count - 1)
        ]
        query_at = iota((2 * tokens, tokens), 0) % tokens
        key_at = iota((2 * tokens, tokens), 1)
        key_taken = jnp.zeros((2 * tokens, tokens), jnp.int32)
        for at in range(iter_count - 1):
            key_taken = jnp.where(key_at // width == at, taken[at], key_taken)
        earlier = (key_at // width < query_at // width) & (key_at % width < key_taken)
        same = (key_at // width == query_at // width) & (key_at <= query_at)
        visible_now = earlier | same
        visible_cache = iota((2 * tokens, cache_slots), 1) < cache_lens[at_batch]
        heads = []
        for head in range(kv_local):
            pair = jnp.concatenate(
                [
                    of_sequence(turned_queries[2 * head], at_batch, 0),
                    of_sequence(turned_queries[2 * head + 1], at_batch, 0),
                ],
                axis=0,
            ).astype(bf16)
            keys_now = of_sequence(turned_keys[head], at_batch, 0).astype(bf16)
            values_now = of_sequence(values, at_batch, head).astype(bf16)

            def weigh(scores, visible):
                scores = score_cap * jnp.tanh(scores / score_cap)
                return jnp.where(visible, jnp.exp(scores), 0.0)

            from_cache = weigh(
                lax.dot_general(pair, cache_keys[at_batch, head], nt, preferred_element_type=f32),
                visible_cache,
            )
            from_now = weigh(
                lax.dot_general(pair, keys_now, nt, preferred_element_type=f32), visible_now
            )
            weight_sum = jnp.sum(from_cache, axis=1, keepdims=True) + jnp.sum(
                from_now, axis=1, keepdims=True
            )
            summed = jnp.dot(
                from_cache.astype(bf16), cache_values[at_batch, head], preferred_element_type=f32
            ) + jnp.dot(from_now.astype(bf16), values_now, preferred_element_type=f32)
            attended = summed / weight_sum
            heads += [attended[:tokens], attended[tokens:]]
        attended_rows.append(jnp.concatenate(heads, axis=1))
    attended = jnp.concatenate(attended_rows, axis=0).astype(bf16)

    ordered = iota((rows, rows), 0)
    wanted = ((ordered // chunk) ^ at_vocab) * chunk + ordered % chunk
    place = iota((rows, rows), 1)
    at_batch = place // tokens
    at_window = (place % tokens) // width
    standing = (at_window * local_batch + at_batch) * width + place % width
    by_sequence = jnp.where(wanted == standing, 1.0, 0.0).astype(bf16)
    by_window = jnp.where(wanted == place, 1.0, 0.0)[:chunk].astype(bf16)
    own[...] = jnp.dot(by_window, gathered.astype(bf16), preferred_element_type=f32).astype(bf16)
    attended = jnp.dot(by_sequence, attended, preferred_element_type=f32).astype(bf16)
    branch = jnp.dot(attended, w_out[...], preferred_element_type=f32)
    keep[...] = branch[:chunk]
    for at, ref in enumerate(sends):
        ref[...] = stacked(branch[(at + 1) * chunk : (at + 2) * chunk]).astype(bf16)


def final_kernel(kept, own, post_gain, final_gain, *refs):
    parts, final = refs[:-1], refs[-1]
    chunk, model_width = kept.shape
    total = jnp.zeros((half_count * chunk, model_width // half_count), f32)
    for part in parts:
        total = total + part[...].astype(f32)
    branch = kept[...] + jnp.concatenate(
        [total[half * chunk : (half + 1) * chunk] for half in range(half_count)], axis=1
    )
    embedded = own[...].astype(f32) * math.sqrt(model_width)
    hidden = embedded + normalize(branch, post_gain[...])
    final[...] = stacked(normalize(hidden, final_gain[...])).astype(bf16)


def join_kernel(*refs):
    parts, joint = refs[:-1], refs[-1]
    joint[...] = jnp.concatenate([part[...].astype(f32) for part in parts], axis=0).astype(bf16)


def half_of_block(parts, half):
    size = parts[0].shape[0]
    chunk = size // half_count
    found = []
    for part in parts:
        values = part[...].astype(f32)
        for at in range(part.shape[0] // size):
            start = at * size + half * chunk
            found.append(values[start : start + chunk])
    return jnp.concatenate(found, axis=0)


def score_blocks(blocks, core_of, order_of, tables, pools):
    vocab_rows = sum(table.shape[0] for table in tables)
    vocab_devices = lax.axis_size("vocab")
    at_vocab = lax.axis_index("vocab")
    at_core = lax.axis_index("batch") % 2
    far = lax.axis_size("batch") // 2
    chunk = blocks[0][0].shape[0] // half_count
    block_rows = chunk * far
    first = (lax.axis_index("batch") * vocab_devices + at_vocab) * vocab_rows
    wanted = []
    for other, order in zip(core_of, order_of):
        owner = owner_of(jnp.int32(order), at_vocab, at_core ^ other)
        parts = []
        for at in range(far):
            pool = pools[2 * at + other : 2 * at + other + 1, :]
            part = jnp.zeros((1, chunk), jnp.int32)
            for place in range(vocab_devices):
                part = jnp.where(
                    owner == place, pool[:, place * chunk : (place + 1) * chunk], part
                )
            parts.append(part)
        wanted.append(jnp.concatenate(parts, axis=1))
    wanted = jnp.concatenate(wanted, axis=1) - first
    values = [
        jnp.concatenate([half_of_block(block, half) for block in blocks], axis=0).astype(bf16)
        for half in range(half_count)
    ]
    wide = values[0].shape[1]
    sums, chosen, largest = [], [], []
    for table in tables:
        raw = jnp.zeros((table.shape[0], values[0].shape[0]), f32)
        for half, value in enumerate(values):
            raw = raw + lax.dot_general(
                table[:, half * wide : (half + 1) * wide],
                value,
                (((1,), (1,)), ((), ())),
                preferred_element_type=f32,
            )
        logits = logit_cap * jnp.tanh(raw / logit_cap)
        sums.append(jnp.sum(jnp.exp(logits), axis=0, keepdims=True))
        hit = iota(logits.shape, 0) == wanted
        chosen.append(jnp.sum(jnp.where(hit, logits, 0.0), axis=0, keepdims=True))
        largest.append(jnp.max(logits, axis=0, keepdims=True))
        wanted = wanted - table.shape[0]
    sums, chosen = sum(sums), sum(chosen)
    top = largest[0]
    for row in largest[1:]:
        top = jnp.maximum(top, row)
    largest = top
    return [
        [row[:, at * block_rows : (at + 1) * block_rows] for at in range(len(blocks))]
        for row in (sums, chosen, largest)
    ]


def score_kernel(orders, halves, parts, *refs):
    pools, scores = refs[-2:]
    tables = refs[len(refs) - 2 - parts : -2]
    count = (len(refs) - parts - 2) // halves
    blocks = [refs[at * halves : (at + 1) * halves] for at in range(count)]
    cores = [0, 1] if len(blocks) > len(orders) else [0]
    core_of = [core for core in cores for _ in orders]
    found = score_blocks(blocks, core_of, orders * len(cores), tables, pools)
    for kind in range(3):
        for at in range(len(blocks)):
            row = kind * len(blocks) + at
            scores[row : row + 1, :] = found[kind][at]


def late_kernel(orders, halves, *refs):
    vocab_devices = lax.axis_size("vocab")
    at_vocab = lax.axis_index("vocab")
    at_batch = lax.axis_index("batch")
    far = lax.axis_size("batch") // 2
    message = refs[-1]
    scores = refs[-2 - len(orders) : -1]
    block, tables, pools = refs[:halves], refs[halves : halves + 2], refs[halves + 2]
    chunk = block[0].shape[0] // half_count
    late = score_blocks([block], [1], [vocab_devices - 1], tables, pools)
    for other in range(2):
        kinds = []
        for kind in range(3):
            found = []
            for group, score in zip(orders, scores):
                row = (kind * 2 + other) * len(group)
                found += [score[row + at : row + at + 1, :] for at in range(len(group))]
            found.append(scores[-1][kind : kind + 1, :] if other == 0 else late[kind][0])
            owners = [
                owner_of(jnp.int32(at), at_vocab, (at_batch % 2) ^ other)
                for at in range(vocab_devices)
            ]
            chunks = []
            for place in range(vocab_devices):
                total = jnp.zeros_like(found[0])
                for at in range(vocab_devices):
                    total = jnp.where(owners[at] == place, found[at], total)
                chunks.append(total)
            kinds.append(jnp.concatenate(chunks, axis=0))
        for at in range(far):
            pieces = [kind[:, at * chunk : (at + 1) * chunk] for kind in kinds]
            pieces.append(jnp.zeros((vocab_devices, lane_count - 3 * chunk), f32))
            piece = jnp.concatenate(pieces, axis=1)
            piece = jnp.concatenate([piece] * vocab_devices, axis=0)
            target = at_batch ^ (2 * at + other)
            size = vocab_devices * vocab_devices
            message[pl.ds(pl.multiple_of(target * size, 8), size), :] = piece


def result_kernel(got, log_total, best_logit, pool_score):
    vocab_devices = lax.axis_size("vocab")
    iter_count, local_batch, width = log_total.shape
    rows = iter_count * local_batch * width
    chunk = rows // vocab_devices
    step = max(8, vocab_devices)
    added = got[0:step, :]
    largest = added
    for at in range(1, got.shape[0] // step):
        part = got[at * step : (at + 1) * step, :]
        added = added + part
        largest = jnp.maximum(largest, part)
    total, top = added[:vocab_devices], largest[:vocab_devices]
    for at in range(1, step // vocab_devices):
        total = total + added[at * vocab_devices : (at + 1) * vocab_devices]
        top = jnp.maximum(top, largest[at * vocab_devices : (at + 1) * vocab_devices])

    def flat(array, kind):
        return jnp.concatenate(
            [array[at : at + 1, kind * chunk : (kind + 1) * chunk] for at in range(vocab_devices)],
            axis=1,
        )

    log_sum = jnp.log(flat(total, 0))
    for ref, found in (
        (log_total, log_sum),
        (best_logit, flat(top, 2)),
        (pool_score, flat(total, 1) - log_sum),
    ):
        for at in range(iter_count):
            for at_batch in range(local_batch):
                start = (at * local_batch + at_batch) * width
                ref[at, at_batch : at_batch + 1, :] = found[:, start : start + width]


def call(kernel, shapes, in_specs, out_specs, flops=0, scratch=(), grant=8):
    return pl.pallas_call(
        kernel,
        out_shape=shapes,
        in_specs=in_specs,
        out_specs=out_specs,
        scratch_shapes=scratch,
        compiler_params=pltpu.CompilerParams(vmem_limit_bytes=grant << 20),
        cost_estimate=pl.CostEstimate(flops=flops, bytes_accessed=flops // 100, transcendentals=0),
    )


def per_device(
    window_ids,
    pool_ids,
    accepted,
    converged,
    cache_lens,
    table,
    attn_gain,
    post_gain,
    final_gain,
    w_query,
    w_key,
    w_value,
    w_out,
    cache_keys,
    cache_values,
):
    iter_count, local_batch, width = window_ids.shape
    vocab_rows, model_width = table.shape
    head_size = cache_keys.shape[3]
    groups = iter_count * local_batch
    rows = groups * width
    batch_devices = lax.axis_size("batch")
    vocab_devices = lax.axis_size("vocab")
    all_devices = batch_devices * vocab_devices
    vocab_bits = bits_of(vocab_devices)
    chunk = rows // vocab_devices
    far = batch_devices // 2

    def shape(*dims, kind=bf16):
        return jax.ShapeDtypeStruct(dims, kind)

    def batch_swap(value, mask):
        return lax.ppermute(value, "batch", [(at, at ^ mask) for at in range(batch_devices)])

    def mixed_swap(value, step):
        pairs = []
        for at in range(all_devices):
            b_at, v_at = divmod(at, vocab_devices)
            bit = vocab_bits[step] if b_at % 2 == 0 else vocab_bits[-1 - step]
            pairs.append((at, b_at * vocab_devices + (v_at ^ bit)))
        return lax.ppermute(value, ("batch", "vocab"), pairs)

    in_hbm = pl.BlockSpec(memory_space=pltpu.HBM)
    own_ids = call(
        pack_kernel,
        shape(2 * groups, width, kind=jnp.int32),
        [in_hbm] * 2,
        vmem,
        scratch=[
            pltpu.VMEM((2, iter_count, local_batch, width), jnp.int32),
            pltpu.SemaphoreType.DMA((2,)),
        ],
        grant=2,
    )(window_ids, pool_ids)
    all_ids = own_ids
    for bit in bits_of(batch_devices):
        all_ids = jnp.concatenate([all_ids, batch_swap(all_ids, bit)], axis=0)

    part_rows = vocab_rows // 2
    tables = []
    for at in range(2):
        tables.append(
            call(
                functools.partial(load_kernel, at * part_rows),
                shape(part_rows, model_width),
                [pl.BlockSpec(memory_space=pl.ANY)],
                vmem,
                flops=10**8,
                scratch=[pltpu.SemaphoreType.DMA(())],
                grant=57,
            )(table)
        )

    def exchange(first_slot):
        *sent, pools, most = call(
            send_kernel,
            [shape(half_count * slots_sent, model_width // half_count)] * far
            + [shape(batch_devices, rows, kind=jnp.int32), shape(1, kind=jnp.int32)],
            [smem, vmem, vmem, vmem],
            [vmem] * (far + 1) + [smem],
            flops=2 * batch_devices * slots_sent * vocab_rows * model_width,
            grant=10,
        )(first_slot, all_ids, *tables)
        got = [sent[0]]
        for mask in range(1, far):
            got.append(batch_swap(sent[mask], 2 * mask))
        other = [batch_swap(part, 1) for part in got]
        placed = call(
            lambda slot, *refs: place_kernel(slot, vocab_rows, *refs),
            [shape(rows, model_width // half_count)] * half_count,
            [smem, vmem] + [vmem] * batch_devices,
            [vmem] * half_count,
            flops=10**8,
        )(first_slot, all_ids, *got, *other)
        return placed, pools, most

    start_slot = jnp.zeros((1,), jnp.int32)
    gathered, pools, most = exchange(start_slot)

    def another_round(state):
        later = state[0] + slots_sent
        return later, [old + new for old, new in zip(state[1], exchange(later)[0])]

    _, gathered = lax.while_loop(
        lambda state: state[0][0] + slots_sent < most[0], another_round, (start_slot, list(gathered))
    )
    for step in range(len(vocab_bits) - 1):
        received = []
        for half in range(half_count):
            received.append(mixed_swap(gathered[half], step))
        gathered = [kept + got for kept, got in zip(gathered, received)]
    received = []
    for half in range(half_count):
        received.append(mixed_swap(gathered[half], len(vocab_bits) - 1))

    half_size = head_size // 2
    freqs = np.float32(10000.0) ** (-np.arange(half_size, dtype=np.float32) / half_size)
    signs = np.concatenate([-np.ones(half_size), np.ones(half_size)]).astype(np.float32)
    cosine, sine = call(
        turn_kernel,
        [shape(rows, head_size, kind=f32)] * 2,
        [smem] * 3 + [vmem] * 2,
        [vmem] * 2,
        flops=10**7,
    )(
        accepted,
        converged,
        cache_lens,
        jnp.asarray(np.concatenate([freqs, freqs])[None]),
        jnp.asarray(signs[None]),
    )

    wide = w_query.shape[1] + w_key.shape[1] + w_value.shape[1]
    keep, own, *sends = call(
        attend_kernel,
        [
            shape(chunk, model_width, kind=f32),
            shape(chunk, model_width),
        ]
        + [shape(half_count * chunk, model_width // half_count)] * (vocab_devices - 1),
        [smem] * 3 + [vmem] * 13,
        [vmem] * (vocab_devices + 1),
        flops=2 * rows * model_width * (wide + w_out.shape[0]),
        grant=20,
    )(
        accepted,
        converged,
        cache_lens,
        *gathered,
        *received,
        cosine,
        sine,
        attn_gain[None],
        w_query,
        w_key,
        w_value,
        w_out,
        cache_keys,
        cache_values,
    )
    branches = []
    for at, send in enumerate(sends):
        pairs = [(place, place ^ (at + 1)) for place in range(vocab_devices)]
        branches.append(lax.ppermute(send, "vocab", pairs))
    final = call(
        final_kernel,
        shape(half_count * chunk, model_width // half_count),
        [vmem] * (len(branches) + 4),
        vmem,
    )(keep, own, post_gain[None], final_gain[None], *branches)

    parts = []
    for mask in range(1, far):
        parts.append(batch_swap(final, 2 * mask))
    joint = call(
        join_kernel,
        shape((far - 2) * half_count * chunk, model_width // half_count),
        [vmem] * (far - 2),
        vmem,
    )(*parts[1:])
    halves = 3
    own_blocks, other_blocks = [], []
    for block in (final, parts[0], joint):
        blocks = [block]
        for step in range(len(vocab_bits)):
            step = len(vocab_bits) - 1 - step
            for at in range(len(blocks)):
                blocks.append(mixed_swap(blocks[at], step))
        own_blocks.append(blocks)
        others = []
        for each in blocks:
            others.append(batch_swap(each, 1))
        other_blocks.append(others)

    per_block = 2 * far * chunk * vocab_rows * model_width

    def halves_of(blocks, orders):
        return [blocks[half][order] for order in orders for half in range(halves)]

    groups_of = [[0], list(range(1, vocab_devices - 1))]
    scores = []
    for orders in groups_of:
        inputs = halves_of(own_blocks, orders) + halves_of(other_blocks, orders)
        scores.append(
            call(
                functools.partial(score_kernel, orders, halves, 2),
                shape(6 * len(orders), far * chunk, kind=f32),
                [vmem] * (len(inputs) + 3),
                vmem,
                flops=2 * per_block * len(orders),
                grant=6 + (16 * len(orders) * far * chunk * model_width >> 20),
            )(*inputs, *tables, pools)
        )
    last = vocab_devices - 1
    scores.append(
        call(
            functools.partial(score_kernel, [last], halves, 2),
            shape(3, far * chunk, kind=f32),
            [vmem] * (halves + 3),
            vmem,
            flops=per_block,
        )(*halves_of(own_blocks, [last]), *tables, pools)
    )
    message = call(
        functools.partial(late_kernel, groups_of, halves),
        shape(all_devices * vocab_devices, lane_count, kind=f32),
        [vmem] * (halves + 3 + len(scores)),
        vmem,
        flops=per_block,
    )(*halves_of(other_blocks, [last]), *tables, pools, *scores)
    totals = lax.all_to_all(message, ("batch", "vocab"), 0, 0, tiled=True)
    return tuple(
        call(
            result_kernel,
            [shape(iter_count, local_batch, width, kind=f32)] * 3,
            [vmem],
            [vmem] * 3,
        )(totals)
    )


def solution(mesh):
    return jax.shard_map(
        per_device,
        mesh=mesh,
        in_specs=(
            P(None, "batch", None),
            P(None, "batch", None),
            P(None, "batch"),
            P(None, "batch"),
            P("batch"),
            P(("batch", "vocab"), None),
            P(),
            P(),
            P(),
            P(None, "vocab"),
            P(None, "vocab"),
            P(None, "vocab"),
            P("vocab", None),
            P("batch", "vocab", None, None),
            P("batch", "vocab", None, None),
        ),
        out_specs=(P(None, "batch", None), P(None, "batch", None), P(None, "batch", None)),
        check_vma=False,
    )
```
